512 devices in a mesh: group: 16 (over y, core), page: 8 (over z), tensor: 4 (over x).
Axes of the slice: x: 4, y: 8, z: 8, core: 2. Of those that a mesh axis runs over, the one named last changes fastest.
Arguments:
- query: bfloat16 [32, 8192], P(None, 'tensor'), may hold values from -400 to 400
- cache_keys: bfloat16 [16384, 16, 1024], P(('group', 'page'), None, 'tensor'), may hold values from -6 to 6
- cache_values: bfloat16 [16384, 16, 1024], P(('group', 'page'), None, 'tensor'), may hold values from -6 to 6
- new_keys: bfloat16 [2048, 16, 1024], P(('group', 'page'), None, 'tensor'), may hold values from -6 to 6
- new_values: bfloat16 [2048, 16, 1024], P(('group', 'page'), None, 'tensor'), may hold values from -6 to 6
- page_map: int32 [2048, 2], replicated, may hold values from 0 to 127, as said below
- page_table: int32 [32, 2048], replicated, may hold values from 0 to 16383, as said below
- lengths: int32 [32], replicated, may hold values from 1009 to 32768, as said below
- out_weight: bfloat16 [8192, 8192], P('tensor', ('group', 'page')), may hold values from -0.0625 to 0.0625
Outputs:
- result: bfloat16 [32, 8192], P(None, ('group', 'page', 'tensor'))
The draws below stay inside these ranges and needn't reach their ends.
Inputs may be any that keep to these rules, and one draw needn't show every extreme that they name: `page_map`: new page r lies on the device of group index r // 128 and page index (r // 16) mod 8; column 0 names the group index of the receiving device at the same page index, column 1 the slot of its cache shard that the page replaces. Of one device's 16 new pages at most 2 go to one receiver, and at every page index one receiver gets exactly 2 from every sender; the slots that one receiver gets are distinct. `page_table`: entry j of row s is the global slot (group index * 8 + page index) * 128 + slot of the j-th page of sequence s. The first ceil(lengths[s] / 16) entries of a row are live; live entries are distinct over all sequences and include every slot named by the page map; the other entries are arbitrary. `lengths`: one sequence has exactly 32768 tokens.
All inputs are finite; a program needn't handle non-finite values.
Results may differ from the reference program's by a relative error of at most 0.0065.
Values may be sent and summed in bfloat16 or wider, within the bound.
A program may use at most 64 MiB of HBM per device.

```python
import math
import jax
import jax.numpy as jnp
from jax import lax

HQ = 64
KVH = 8
HD = 128
D = 8192
PAGE = 16
SLOTS = 128
NEW_DEV = 16
CAP = 2
SEQS = 32
SHARDS = 128
NEW_ALL = 2048
SLOTS_ALL = 16384
AVG_PAGES = 512
MAXP = 2048
N_GROUP = 16
N_PAGE = 8


def layout(key):
    subkeys = jax.random.split(key, 9)
    choices_all = N_GROUP * CAP
    column = jnp.arange(SHARDS, dtype=jnp.int32) % N_PAGE
    hottest = jax.random.randint(subkeys[0], (N_PAGE,), 0, N_GROUP, dtype=jnp.int32)
    favour = jax.random.randint(subkeys[1], (N_PAGE, N_GROUP), 0, 4, dtype=jnp.int32)
    choice_target = jnp.arange(choices_all, dtype=jnp.int32) // CAP
    jitter = jax.random.randint(subkeys[2], (SHARDS, choices_all), 0, 1024, dtype=jnp.int32)
    favour_boost = favour[column][:, choice_target] * 1024
    hot_boost = (choice_target[None, :] == hottest[column][:, None]).astype(jnp.int32) * 8192
    priority = (jitter + favour_boost + hot_boost) * choices_all + jnp.arange(choices_all, dtype=jnp.int32)[None, :]
    chosen = lax.top_k(priority, NEW_DEV)[1].astype(jnp.int32)
    target = chosen // CAP
    receiver = (target * N_PAGE + column[:, None]).reshape(-1)
    receiver_hits = (receiver[:, None] == jnp.arange(SHARDS, dtype=jnp.int32)[None, :]).astype(jnp.int32)
    before = jnp.sum((jnp.cumsum(receiver_hits, axis=0) - receiver_hits) * receiver_hits, axis=1)
    slot_priority = jax.random.randint(subkeys[3], (SHARDS, SLOTS), 0, 1024, dtype=jnp.int32) * SLOTS + jnp.arange(SLOTS, dtype=jnp.int32)[None, :]
    shuffles = jnp.argsort(slot_priority, axis=1).astype(jnp.int32)
    slot_number = shuffles[receiver, before]
    page_map = jnp.stack([target.reshape(-1), slot_number], axis=1).astype(jnp.int32)
    fresh_slots = receiver * SLOTS + slot_number
    counts = jax.random.randint(subkeys[4], (SEQS,), AVG_PAGES // 8, AVG_PAGES * 7 // 8, dtype=jnp.int32)
    longest = jax.random.randint(subkeys[5], (), 0, SEQS, dtype=jnp.int32)
    is_long = jnp.arange(SEQS, dtype=jnp.int32) == longest
    counts = jnp.where(is_long, MAXP, counts)
    last_fill = jax.random.randint(subkeys[6], (SEQS,), 1, PAGE + 1, dtype=jnp.int32)
    last_fill = jnp.where(is_long, PAGE, last_fill)
    lengths = ((counts - 1) * PAGE + last_fill).astype(jnp.int32)
    is_fresh = jnp.zeros((SLOTS_ALL,), jnp.int32).at[fresh_slots].set(1)
    ordering_key = jax.random.randint(subkeys[7], (SLOTS_ALL,), 0, 1024, dtype=jnp.int32) * SLOTS_ALL + jnp.arange(SLOTS_ALL, dtype=jnp.int32) - is_fresh * (1024 * SLOTS_ALL)
    ordering = jnp.argsort(ordering_key).astype(jnp.int32)
    starts = jnp.cumsum(counts) - counts
    page_index = jnp.arange(MAXP, dtype=jnp.int32)
    picked = jnp.minimum(starts[:, None] + page_index[None, :], SLOTS_ALL - 1)
    filler = jax.random.randint(subkeys[8], (SEQS, MAXP), 0, SLOTS_ALL, dtype=jnp.int32)
    page_rows = jnp.where(page_index[None, :] < counts[:, None], ordering[picked], filler).astype(jnp.int32)
    return (page_map, page_rows, lengths)


def draw_page_map(key, part):
    return layout(jax.random.fold_in(key, 11))[0]


def draw_page_table(key, part):
    return layout(jax.random.fold_in(key, 11))[1]


def draw_lengths(key, part):
    return layout(jax.random.fold_in(key, 11))[2]


def draw_query(key, part):
    first_key, second_key = jax.random.split(jax.random.fold_in(key, 23))
    base = jax.random.normal(first_key, (SEQS, HQ, HD), dtype=jnp.float32)
    spread = jax.random.uniform(second_key, (SEQS, HQ, 1), dtype=jnp.float32, minval=0.0, maxval=math.log(16.0))
    values = jnp.clip(base * jnp.exp(spread), -400.0, 400.0)
    return values.reshape(SEQS, HQ * HD).astype(jnp.bfloat16)


def level_of(rng, dims, cuts, least, largest):
    loudness, own = 1.0, jax.random.fold_in(rng, 6)
    for axis_at, blocks in cuts:
        draws = jnp.exp(jax.random.uniform(jax.random.fold_in(own, axis_at), (blocks,), jnp.float32, least / len(cuts), largest / len(cuts)))
        loudness = loudness * jnp.repeat(draws, dims[axis_at] // blocks).reshape([-1 if axis == axis_at else 1 for axis in range(len(dims))])
    return loudness


def gaussian(own_key, extent, scale, most, shards=(), kind=jnp.bfloat16):
    result = jax.random.normal(own_key, extent, jnp.float32) * scale
    if len(shards) > 0:
        result = level_of(own_key, extent, shards, -0.22, 0.18) * result
    return jnp.clip(result, min=-most, max=most).astype(kind)


def setup_inputs(seed: int = 0) -> dict:
    splits = jax.random.split(jax.random.key(seed), 10)
    query = draw_query(jax.random.fold_in(splits[9], 71), 0)
    cache_keys = gaussian(splits[1], (SLOTS_ALL, PAGE, KVH * HD), 1.0, 6.0, ((0, 128), (2, 4)))
    cache_values = gaussian(splits[2], (SLOTS_ALL, PAGE, KVH * HD), 1.0, 6.0, ((0, 128), (2, 4)))
    new_keys = gaussian(splits[3], (NEW_ALL, PAGE, KVH * HD), 1.0, 6.0, ((0, 128), (2, 4)))
    new_values = gaussian(splits[4], (NEW_ALL, PAGE, KVH * HD), 1.0, 6.0, ((0, 128), (2, 4)))
    page_map = draw_page_map(jax.random.fold_in(splits[9], 71), 0)
    page_table = draw_page_table(jax.random.fold_in(splits[9], 71), 0)
    lengths = draw_lengths(jax.random.fold_in(splits[9], 71), 0)
    out_weight = gaussian(splits[8], (HQ * HD, D), (HQ * HD) ** -0.5, 0.0625, ((0, 4), (1, 128)))
    return dict(query=query, cache_keys=cache_keys, cache_values=cache_values, new_keys=new_keys, new_values=new_values, page_map=page_map, page_table=page_table, lengths=lengths, out_weight=out_weight)


very_low = -1.0e30


def attend(page_row, length, query_row, key_cache, value_cache):
    share = HQ // KVH
    shard_of = jnp.repeat(page_row // SLOTS, PAGE).astype(jnp.int32)
    key_rows = key_cache[page_row].reshape(MAXP * PAGE, KVH, HD).astype(jnp.float32)
    value_rows = value_cache[page_row].reshape(MAXP * PAGE, KVH, HD).astype(jnp.float32)
    query_heads = query_row.reshape(KVH, share, HD).astype(jnp.float32)
    scores = jnp.einsum("kgd,tkd->kgt", query_heads, key_rows) * (HD ** -0.5)
    visible = jnp.arange(MAXP * PAGE, dtype=jnp.int32) < length
    scores = jnp.where(visible, scores, very_low)
    shard_high = jnp.full((SHARDS, KVH, share), very_low, dtype=jnp.float32)
    shard_high = shard_high.at[shard_of].max(jnp.moveaxis(scores, 2, 0))
    local_high = jnp.moveaxis(shard_high[shard_of], 0, 2)
    overall = jnp.max(scores, axis=2, keepdims=True)
    raw_weights = jnp.where(visible, jnp.exp(scores - local_high), 0.0)
    rounded = lax.optimization_barrier(raw_weights.astype(jnp.bfloat16)).astype(jnp.float32)
    factor = jnp.exp(local_high - overall)
    total = jnp.sum(raw_weights * factor, axis=2)
    summed = jnp.einsum("kgt,tkd->kgd", rounded * factor, value_rows)
    return (summed / total[..., None]).reshape(HQ * HD).astype(jnp.bfloat16)


def reference(query, cache_keys, cache_values, new_keys, new_values, page_map, page_table, lengths, out_weight):
    row_ids = jnp.arange(NEW_ALL, dtype=jnp.int32)
    column = (row_ids // NEW_DEV) % N_PAGE
    target = ((page_map[:, 0] * N_PAGE + column) * SLOTS + page_map[:, 1]).astype(jnp.int32)
    key_cache = cache_keys.at[target].set(new_keys)
    value_cache = cache_values.at[target].set(new_values)

    def one_sequence(bundle):
        return attend(bundle[0], bundle[1], bundle[2], key_cache, value_cache)

    attention = lax.map(one_sequence, (page_table, lengths, query))
    return jnp.dot(attention, out_weight, preferred_element_type=jnp.float32).astype(jnp.bfloat16)
```

```python
import functools
import math

import jax
import jax.numpy as jnp
from jax import lax
from jax.experimental import pallas as pl
from jax.experimental.pallas import tpu as pltpu
from jax.sharding import PartitionSpec as P

HD = 128
PAGE = 16
LANES = 128
CORES = 2
MESH = pl.DeviceIdType.MESH
VERY_LOW = -1.0e30
SCALE2 = HD**-0.5 * math.log2(math.e)
NT = (((1,), (1,)), ((), ()))


def lanes_of(shape):
    return lax.broadcasted_iota(jnp.int32, shape, len(shape) - 1)


def rows_of(shape):
    return lax.broadcasted_iota(jnp.int32, shape, len(shape) - 2)


def lane_sum(x):
    return jnp.sum(x.astype(jnp.float32), axis=1, keepdims=True).astype(jnp.int32)


def lane_or(words):
    low = lane_sum(words & 0xFFFF)
    high = lane_sum(lax.shift_right_logical(words, 16) & 0xFFFF)
    return low, high


def build_bias(tbl, pm, lens, tgt, bias, gi, z, n_page, slots, new_dev):
    seqs, pages = tbl.shape
    total = pm.shape[1]
    shard = gi * n_page + z
    base = shard * slots
    eye = rows_of((seqs, seqs)) == lanes_of((seqs, seqs))
    length = lane_sum(jnp.where(eye, lens[...], 0))
    used = (length + (PAGE - 1)) >> 4
    fill = length - (used - 1) * PAGE
    target = pm[0:1, :]
    slot = pm[1:2, :]
    number = lanes_of((1, total))
    sheet = (number // new_dev) % n_page
    valid = (target == gi) & (sheet == z)
    off = shard * new_dev
    own = jnp.where(
        lanes_of((new_dev, total)) == rows_of((new_dev, total)) + off,
        (target * n_page + z) * slots + slot,
        0,
    )
    tgt[...] = jnp.broadcast_to(lane_sum(own), tgt.shape)
    stale = []
    for w in range(slots // 16):
        hit = valid & ((slot >> 4) == w)
        stale.append(lane_sum(jnp.where(hit, jnp.int32(1) << (slot & 15), 0)))
    shape = (seqs, LANES)
    used_b = jnp.broadcast_to(used, shape)
    words = [jnp.zeros(shape, jnp.int32) for _ in range(slots // 32)]
    fresh = jnp.zeros(shape, jnp.int32)
    last = jnp.zeros(shape, jnp.int32)
    marks = [jnp.broadcast_to(tgt[k : k + 1, :], shape) for k in range(new_dev)]
    for c in range(pages // LANES):
        entry = tbl[:, c * LANES : (c + 1) * LANES]
        j = lanes_of(shape) + c * LANES
        last = last + jnp.where(j == used_b - 1, entry, 0)
        entry = jnp.where(j < used_b, entry, -1)
        local = entry - base
        high = local >> 5
        bit = jnp.int32(1) << (local & 31)
        for w in range(slots // 32):
            words[w] = words[w] | jnp.where(high == w, bit, 0)
        for k in range(new_dev):
            fresh = fresh | jnp.where(entry == marks[k], 1 << k, 0)
    last_b = jnp.broadcast_to(lane_sum(last), shape)
    fill_b = jnp.broadcast_to(fill, shape)
    owned = []
    for w in range(slots // 32):
        owned.extend(lane_or(words[w]))
    fresh_b = jnp.broadcast_to(lane_sum(fresh), shape)
    last_fresh = jnp.zeros(shape, jnp.int32)
    for k in range(new_dev):
        last_fresh = last_fresh | jnp.where(last_b == marks[k], 1 << k, 0)
    lane = lanes_of(shape)
    tail_end = (last_b - base) * PAGE + PAGE
    tail_start = tail_end - PAGE + fill_b
    per_tile = LANES // PAGE
    for w in range(slots // 16):
        word = jnp.broadcast_to(owned[w] & ~stale[w], shape)
        for half in range(16 // per_tile):
            c = w * (16 // per_tile) + half
            token = lane + c * LANES
            here = (lax.shift_right_logical(word, (lane >> 4) + half * per_tile) & 1) == 1
            here = here & ((token < tail_start) | (token >= tail_end))
            bias[:, c * LANES : (c + 1) * LANES] = jnp.where(here, 0.0, VERY_LOW)
    first = slots * PAGE
    for c in range(new_dev // per_tile):
        shift = (lane >> 4) + c * per_tile
        here = (lax.shift_right_logical(fresh_b, shift) & 1) == 1
        ends = (lax.shift_right_logical(last_fresh, shift) & 1) == 1
        here = here & ~(ends & ((lane & 15) >= fill_b))
        bias[:, first + c * LANES : first + (c + 1) * LANES] = jnp.where(here, 0.0, VERY_LOW)


def merge(stat_rows, values, rows):
    count = len(stat_rows)
    pad = [jnp.zeros((-count % 8, LANES), jnp.float32)] if count % 8 else []
    stats = jnp.concatenate(stat_rows + pad, axis=0)
    real = rows_of(stats.shape) < count
    highest = jnp.max(jnp.where(real, stats, -jnp.inf), axis=0, keepdims=True)
    in_max = lanes_of(stats.shape) < rows
    factor = jnp.where(real & in_max, jnp.exp2(jnp.where(in_max, stats - highest, 0.0)), 0.0)
    sums = pltpu.roll(stats, LANES - rows, 1)
    total = jnp.sum(factor * jnp.where(in_max, sums, 0.0), axis=0, keepdims=True)
    square = jnp.concatenate(
        [factor, jnp.broadcast_to(total, (8, LANES)), jnp.zeros((LANES - 8 - stats.shape[0], LANES), jnp.float32)],
        axis=0,
    )
    across = square.T
    mixed = across[:rows, 0:1] * values[0].astype(jnp.float32)
    for k in range(1, count):
        mixed = mixed + across[:rows, k : k + 1] * values[k].astype(jnp.float32)
    total_column = across[:rows, stats.shape[0] : stats.shape[0] + 1]
    return highest, total, total_column, mixed


def kernel(
    dims,
    q_in,
    ck_in,
    cv_in,
    nk_in,
    nv_in,
    pm_in,
    tbl_in,
    len_in,
    w_in,
    out_ref,
    q,
    key,
    value,
    pm,
    tbl,
    lens,
    weight,
    tgt,
    bias,
    scores,
    probs,
    tops,
    part_a,
    part_b,
    stat_a,
    stat_b,
    got_a,
    got_b,
    gots_a,
    gots_b,
    mid_a,
    mid_b,
    mids_a,
    mids_b,
    gotm_a,
    gotm_b,
    gotms_a,
    gotms_b,
    att_a,
    att_b,
    last_out,
    last_in,
    local_sem,
    send_sem,
    recv_sem,
):
    n_group, n_page, n_tensor, slots, new_dev = dims
    n_y = n_group // CORES
    gi = lax.axis_index("group")
    z = lax.axis_index("page")
    x = lax.axis_index("tensor")
    y = gi // CORES
    core = gi % CORES
    seqs = q.shape[0]
    kv_heads = key.shape[1] // HD
    share = q.shape[1] // HD // kv_heads
    rows = share * seqs
    cache_rows = slots * PAGE

    copies = []

    def fetch(src, dst):
        copy = pltpu.make_async_copy(src, dst, local_sem.at[len(copies)])
        copy.start()
        copies.append(copy)

    fetch(len_in, lens)
    fetch(pm_in, pm)
    fetch(tbl_in, tbl)
    fetch(q_in, q)
    fetch(ck_in, key.at[pl.ds(0, cache_rows)])
    fetch(nk_in, key.at[pl.ds(cache_rows, new_dev * PAGE)])
    fetch(cv_in, value.at[pl.ds(0, cache_rows)])
    fetch(nv_in, value.at[pl.ds(cache_rows, new_dev * PAGE)])
    fetch(w_in, weight)

    def along_group(d):
        return {"group": (gi + d) % n_group}

    def along_sheet(d):
        other = (z * CORES + core + d) % (n_page * CORES)
        return {"group": y * CORES + other % CORES, "page": other // CORES}

    def along_page(d):
        return {"page": (z + d) % n_page}

    def along_y(d):
        return {"group": (y + d) % n_y * CORES + core}

    def along_tensor(d):
        return {"tensor": (x + d) % n_tensor}

    n_sheet = n_page * CORES
    place_b = z * CORES + core
    greeted = [along_group(d) for d in range(1, n_group)]
    for d in range(1, n_sheet):
        if d % CORES == 0:
            greeted.append(along_sheet(d))
    greeted_cross = [d for d in range(1, n_sheet) if d % CORES]
    greeted += [along_tensor(d) for d in range(1, n_tensor)]
    barrier = pltpu.get_barrier_semaphore()
    for peer in greeted:
        pl.semaphore_signal(barrier, inc=1, device_id=peer, device_id_type=MESH)
    for d in greeted_cross:
        pl.semaphore_signal(barrier, inc=1, device_id=along_sheet(d), device_id_type=MESH)

    used = [0]

    def send(src, dst, peer):
        at = used[0]
        used[0] += 1
        copy = pltpu.make_async_remote_copy(
            src_ref=src,
            dst_ref=dst,
            send_sem=send_sem.at[at],
            recv_sem=recv_sem.at[at],
            device_id=peer,
            device_id_type=MESH,
        )
        copy.start()
        return copy

    for k in range(3):
        copies[k].wait()
    build_bias(tbl, pm, lens, tgt, bias, gi, z, n_page, slots, new_dev)
    for k in range(3, 6):
        copies[k].wait()
    for half in range(kv_heads):
        heads = range(half * share, (half + 1) * share)
        stacked = jnp.concatenate([q[:, h * HD : (h + 1) * HD] for h in heads], axis=0)
        scores[half] = lax.dot_general(
            stacked,
            key[:, half * HD : (half + 1) * HD],
            NT,
            preferred_element_type=jnp.float32,
        )
    for k in range(6, 8):
        copies[k].wait()

    def far_first(count):
        return sorted(range(1, count), key=lambda d: -min(d, count - d))

    def attend(half, part, stat):
        count, own_rows = part.shape[0], part.shape[1]
        block = 16
        for b in range(rows // block):
            s0 = b * block % seqs
            s = scores[half, b * block : (b + 1) * block, :] * SCALE2 + bias[s0 : s0 + block, :]
            top = jnp.max(s, axis=1, keepdims=True)
            probs[b * block : (b + 1) * block, :] = jnp.exp2(s - top).astype(jnp.bfloat16)
            tops[b * block : (b + 1) * block, :] = jnp.broadcast_to(top, (block, LANES))
        v = value[:, half * HD : (half + 1) * HD]
        wide = jnp.concatenate([v, jnp.ones_like(v)], axis=1)
        summed = jnp.dot(probs[...], wide, preferred_element_type=jnp.float32)
        shape = (own_rows, LANES)
        lane, row = lanes_of(shape), rows_of(shape)
        for k in range(count):
            at = slice(k * own_rows, (k + 1) * own_rows)
            part[k] = summed[at, :HD].astype(jnp.bfloat16)
            picked = jnp.where(lane == row, tops[at, :], jnp.where(lane == row + own_rows, summed[at, HD:], 0.0))
            stat[k] = jnp.sum(picked, axis=0, keepdims=True)

    def scatter(part, stat, got, gots, place, peer_of):
        count = part.shape[0]
        sent = {}
        for d in far_first(count):
            owner = (place + d) % count
            sent[d] = (
                send(part.at[owner], got.at[d - 1], peer_of(d)),
                send(stat.at[owner], gots.at[d - 1], peer_of(d)),
            )
        return sent

    def merge_scattered(sent, part, stat, got, gots, mid, mids, place):
        own_rows = part.shape[1]
        for d in sent:
            for copy in sent[d]:
                copy.wait_recv()
        stats = [stat[place]] + [gots[d - 1] for d in sorted(sent)]
        values = [part[place]] + [got[d - 1] for d in sorted(sent)]
        highest, total, _, mixed = merge(stats, values, own_rows)
        mid[...] = mixed.astype(jnp.bfloat16)
        low = lanes_of((1, LANES)) < own_rows
        mids[...] = jnp.where(low, highest, pltpu.roll(total, own_rows, 1))

    def spread(mid, mids, gotm, gotms, peer_of):
        sent = {}
        for d in far_first(gotm.shape[0] + 1):
            sent[d] = (send(mid, gotm.at[d - 1], peer_of(d)), send(mids, gotms.at[d - 1], peer_of(d)))
        return sent

    def merge_spread(sent, mid, mids, gotm, gotms, att, place):
        for d in sent:
            for copy in sent[d]:
                copy.wait_recv()
        stats = [mids[...]] + [gotms[d - 1] for d in sorted(sent)]
        values = [mid[...]] + [gotm[d - 1] for d in sorted(sent)]
        _, _, total_column, mixed = merge(stats, values, mid.shape[0])
        att[place] = (mixed / total_column).astype(jnp.bfloat16)

    def gather(att, place, peer_of):
        return {d: (send(att.at[place], att.at[place], peer_of(d)),) for d in far_first(att.shape[0])}

    def finish(sent):
        for d in sent:
            for copy in sent[d]:
                copy.wait_send()

    attend(0, part_a, stat_a)
    pl.semaphore_wait(barrier, len(greeted) + len(greeted_cross))
    first_a = scatter(part_a, stat_a, got_a, gots_a, gi, along_group)
    attend(1, part_b, stat_b)
    first_b = scatter(part_b, stat_b, got_b, gots_b, place_b, along_sheet)
    merge_scattered(first_a, part_a, stat_a, got_a, gots_a, mid_a, mids_a, gi)
    second_a = spread(mid_a, mids_a, gotm_a, gotms_a, along_page)
    merge_scattered(first_b, part_b, stat_b, got_b, gots_b, mid_b, mids_b, place_b)
    second_b = spread(mid_b, mids_b, gotm_b, gotms_b, along_y)
    finish(first_a)
    finish(first_b)
    merge_spread(second_a, mid_a, mids_a, gotm_a, gotms_a, att_a, gi)
    third_a = gather(att_a, gi, along_group)
    merge_spread(second_b, mid_b, mids_b, gotm_b, gotms_b, att_b, place_b)
    third_b = gather(att_b, place_b, along_sheet)
    finish(second_a)
    finish(second_b)
    copies[8].wait()
    for sent in (third_a, third_b):
        for d in sent:
            for copy in sent[d]:
                copy.wait_recv()
    pieces = []
    for att in (att_a, att_b):
        flat = att[...].reshape(rows, HD)
        pieces += [flat[h * seqs : (h + 1) * seqs] for h in range(share)]
    features = jnp.concatenate(pieces, axis=1)
    last_out[...] = lax.dot_general(features, weight[...], NT, preferred_element_type=jnp.float32)
    fourth = {d: (send(last_out, last_in.at[d - 1], along_tensor(d)),) for d in far_first(n_tensor)}
    finish(third_a)
    finish(third_b)
    for d in fourth:
        for copy in fourth[d]:
            copy.wait_recv()
    result = last_out[...]
    for d in range(1, n_tensor):
        result = result + last_in[d - 1]
    width = out_ref.shape[1]
    mine = result[:, :width]
    for t in range(1, n_tensor):
        mine = jnp.where(x == t, result[:, t * width : (t + 1) * width], mine)
    out_ref[...] = mine.astype(out_ref.dtype)
    finish(fourth)


def on_device(sizes, query, cache_keys, cache_values, new_keys, new_values, page_map, page_table, lengths, out_weight):
    n_group, n_page, n_tensor = sizes
    slots, page, width = cache_keys.shape
    new_dev = new_keys.shape[0]
    seqs = query.shape[0]
    tokens = (slots + new_dev) * page
    kv_heads = width // HD
    share = query.shape[1] // HD // kv_heads
    rows = share * seqs
    n_sheet = n_page * CORES
    n_y = n_group // CORES
    columns = out_weight.shape[1]
    rows_a, rows_b = rows // n_group, rows // n_sheet
    bf16, f32 = jnp.bfloat16, jnp.float32
    copies = 2 * (n_group - 1) + 2 * (n_sheet - 1) + 2 * (n_page - 1) + 2 * (n_y - 1)
    copies += (n_group - 1) + (n_sheet - 1) + (n_tensor - 1)
    scratch = [
        pltpu.VMEM(query.shape, bf16),
        pltpu.VMEM((tokens, width), bf16),
        pltpu.VMEM((tokens, width), bf16),
        pltpu.VMEM((2, page_map.shape[0]), jnp.int32),
        pltpu.VMEM(page_table.shape, jnp.int32),
        pltpu.VMEM((1, seqs), jnp.int32),
        pltpu.VMEM((columns, out_weight.shape[0]), bf16),
        pltpu.VMEM((new_dev, LANES), jnp.int32),
        pltpu.VMEM((seqs, tokens), f32),
        pltpu.VMEM((kv_heads, rows, tokens), f32),
        pltpu.VMEM((rows, tokens), bf16),
        pltpu.VMEM((rows, LANES), f32),
        pltpu.VMEM((n_group, rows_a, HD), bf16),
        pltpu.VMEM((n_sheet, rows_b, HD), bf16),
        pltpu.VMEM((n_group, 1, LANES), f32),
        pltpu.VMEM((n_sheet, 1, LANES), f32),
        pltpu.VMEM((n_group - 1, rows_a, HD), bf16),
        pltpu.VMEM((n_sheet - 1, rows_b, HD), bf16),
        pltpu.VMEM((n_group - 1, 1, LANES), f32),
        pltpu.VMEM((n_sheet - 1, 1, LANES), f32),
        pltpu.VMEM((rows_a, HD), bf16),
        pltpu.VMEM((rows_b, HD), bf16),
        pltpu.VMEM((1, LANES), f32),
        pltpu.VMEM((1, LANES), f32),
        pltpu.VMEM((n_page - 1, rows_a, HD), bf16),
        pltpu.VMEM((n_y - 1, rows_b, HD), bf16),
        pltpu.VMEM((n_page - 1, 1, LANES), f32),
        pltpu.VMEM((n_y - 1, 1, LANES), f32),
        pltpu.VMEM((n_group, rows_a, HD), bf16),
        pltpu.VMEM((n_sheet, rows_b, HD), bf16),
        pltpu.VMEM((seqs, columns), f32),
        pltpu.VMEM((n_tensor - 1, seqs, columns), f32),
        pltpu.SemaphoreType.DMA((9,)),
        pltpu.SemaphoreType.DMA((copies,)),
        pltpu.SemaphoreType.DMA((copies,)),
    ]
    return pl.pallas_call(
        functools.partial(kernel, (n_group, n_page, n_tensor, slots, new_dev)),
        out_shape=jax.ShapeDtypeStruct((seqs, columns // n_tensor), bf16),
        in_specs=[pl.BlockSpec(memory_space=pl.ANY)] * 9,
        out_specs=pl.BlockSpec(memory_space=pltpu.VMEM),
        scratch_shapes=scratch,
        compiler_params=pltpu.CompilerParams(
            collective_id=0, has_side_effects=True, vmem_limit_bytes=40 * 1024 * 1024
        ),
    )(
        query,
        cache_keys.reshape(slots * page, width),
        cache_values.reshape(slots * page, width),
        new_keys.reshape(new_dev * page, width),
        new_values.reshape(new_dev * page, width),
        page_map.T,
        page_table,
        lengths.reshape(1, seqs),
        out_weight.T,
    )


def solution(mesh):
    shards = ("group", "page")
    sizes = (mesh.shape["group"], mesh.shape["page"], mesh.shape["tensor"])
    placed = (
        P(None, "tensor"),
        P(shards, None, "tensor"),
        P(shards, None, "tensor"),
        P(shards, None, "tensor"),
        P(shards, None, "tensor"),
        P(),
        P(),
        P(),
        P("tensor", shards),
    )
    return jax.shard_map(
        functools.partial(on_device, sizes),
        mesh=mesh,
        in_specs=placed,
        out_specs=P(None, ("group", "page", "tensor")),
        check_vma=False,
    )
```

```python
import functools
import math

import jax
import jax.numpy as jnp
from jax import lax
from jax.experimental import pallas as pl
from jax.experimental.pallas import tpu as pltpu
from jax.sharding import PartitionSpec as P

HD = 128
PAGE = 16
LANES = 128
CORES = 2
MESH = pl.DeviceIdType.MESH
VERY_LOW = -1.0e30
SCALE2 = HD**-0.5 * math.log2(math.e)
NT = (((1,), (1,)), ((), ()))


def lanes_of(shape):
    return lax.broadcasted_iota(jnp.int32, shape, len(shape) - 1)


def rows_of(shape):
    return lax.broadcasted_iota(jnp.int32, shape, len(shape) - 2)


def lane_sum(x):
    return jnp.sum(x.astype(jnp.float32), axis=1, keepdims=True).astype(jnp.int32)


def lane_or(words):
    low = lane_sum(words & 0xFFFF)
    high = lane_sum(lax.shift_right_logical(words, 16) & 0xFFFF)
    return low, high


def build_bias(tbl, pm, lens, tgt, bias, gi, z, n_page, slots, new_dev):
    seqs, pages = tbl.shape
    total = pm.shape[1]
    shard = gi * n_page + z
    base = shard * slots
    eye = rows_of((seqs, seqs)) == lanes_of((seqs, seqs))
    length = lane_sum(jnp.where(eye, lens[...], 0))
    used = (length + (PAGE - 1)) >> 4
    fill = length - (used - 1) * PAGE
    target = pm[0:1, :]
    slot = pm[1:2, :]
    number = lanes_of((1, total))
    sheet = (number // new_dev) % n_page
    valid = (target == gi) & (sheet == z)
    off = shard * new_dev
    own = jnp.where(
        lanes_of((new_dev, total)) == rows_of((new_dev, total)) + off,
        (target * n_page + z) * slots + slot,
        0,
    )
    tgt[...] = jnp.broadcast_to(lane_sum(own), tgt.shape)
    stale = []
    for w in range(slots // 16):
        hit = valid & ((slot >> 4) == w)
        stale.append(lane_sum(jnp.where(hit, jnp.int32(1) << (slot & 15), 0)))
    shape = (seqs, LANES)
    used_b = jnp.broadcast_to(used, shape)
    words = [jnp.zeros(shape, jnp.int32) for _ in range(slots // 32)]
    fresh = jnp.zeros(shape, jnp.int16)
    last = jnp.zeros(shape, jnp.int32)
    marks = [jnp.broadcast_to(tgt[k : k + 1, :], shape) for k in range(new_dev)]
    narrow_marks = [m.astype(jnp.int16) for m in marks]
    narrow_bits = [jnp.int16((1 << k) if k < 15 else -(1 << 15)) for k in range(new_dev)]
    for c in range(pages // LANES):
        entry = tbl[:, c * LANES : (c + 1) * LANES]
        j = lanes_of(shape) + c * LANES
        last = last + jnp.where(j == used_b - 1, entry, 0)
        entry = jnp.where(j < used_b, entry, -1)
        local = entry - base
        high = local >> 5
        bit = jnp.int32(1) << (local & 31)
        for w in range(slots // 32):
            words[w] = words[w] | jnp.where(high == w, bit, 0)
        narrow = entry.astype(jnp.int16)
        for k in range(new_dev):
            fresh = fresh | jnp.where(narrow == narrow_marks[k], narrow_bits[k], jnp.int16(0))
    last_b = jnp.broadcast_to(lane_sum(last), shape)
    fill_b = jnp.broadcast_to(fill, shape)
    owned = []
    for w in range(slots // 32):
        owned.extend(lane_or(words[w]))
    fresh_b = jnp.broadcast_to(lane_sum(fresh.astype(jnp.int32) & 0xFFFF), shape)
    last_fresh = jnp.zeros(shape, jnp.int32)
    for k in range(new_dev):
        last_fresh = last_fresh | jnp.where(last_b == marks[k], 1 << k, 0)
    lane = lanes_of(shape)
    tail_end = (last_b - base) * PAGE + PAGE
    tail_start = tail_end - PAGE + fill_b
    per_tile = LANES // PAGE
    for w in range(slots // 16):
        word = jnp.broadcast_to(owned[w] & ~stale[w], shape)
        for half in range(16 // per_tile):
            c = w * (16 // per_tile) + half
            token = lane + c * LANES
            here = (lax.shift_right_logical(word, (lane >> 4) + half * per_tile) & 1) == 1
            here = here & ((token < tail_start) | (token >= tail_end))
            bias[:, c * LANES : (c + 1) * LANES] = jnp.where(here, 0.0, VERY_LOW)
    first = slots * PAGE
    for c in range(new_dev // per_tile):
        shift = (lane >> 4) + c * per_tile
        here = (lax.shift_right_logical(fresh_b, shift) & 1) == 1
        ends = (lax.shift_right_logical(last_fresh, shift) & 1) == 1
        here = here & ~(ends & ((lane & 15) >= fill_b))
        bias[:, first + c * LANES : first + (c + 1) * LANES] = jnp.where(here, 0.0, VERY_LOW)


def merge(stat_rows, values, rows):
    count = len(stat_rows)
    pad = [jnp.zeros((-count % 8, LANES), jnp.float32)] if count % 8 else []
    stats = jnp.concatenate(stat_rows + pad, axis=0)
    real = rows_of(stats.shape) < count
    highest = jnp.max(jnp.where(real, stats, -jnp.inf), axis=0, keepdims=True)
    in_max = lanes_of(stats.shape) < rows
    factor = jnp.where(real & in_max, jnp.exp2(jnp.where(in_max, stats - highest, 0.0)), 0.0)
    sums = pltpu.roll(stats, LANES - rows, 1)
    total = jnp.sum(factor * jnp.where(in_max, sums, 0.0), axis=0, keepdims=True)
    square = jnp.concatenate(
        [factor, jnp.broadcast_to(total, (8, LANES)), jnp.zeros((LANES - 8 - stats.shape[0], LANES), jnp.float32)],
        axis=0,
    )
    across = square.T
    mixed = across[:rows, 0:1] * values[0].astype(jnp.float32)
    for k in range(1, count):
        mixed = mixed + across[:rows, k : k + 1] * values[k].astype(jnp.float32)
    total_column = across[:rows, stats.shape[0] : stats.shape[0] + 1]
    return highest, total, total_column, mixed


def kernel(
    dims,
    q_in,
    ck_in,
    cv_in,
    nk_in,
    nv_in,
    pm_in,
    tbl_in,
    len_in,
    w_in,
    out_ref,
    q,
    key,
    value,
    pm,
    tbl,
    lens,
    weight,
    tgt,
    bias,
    scores,
    probs,
    tops,
    part_a,
    part_b,
    stat_a,
    stat_b,
    got_a,
    got_b,
    gots_a,
    gots_b,
    mid_a,
    mid_b,
    mids_a,
    mids_b,
    gotm_a,
    gotm_b,
    gotms_a,
    gotms_b,
    att_a,
    att_b,
    last_out,
    last_in,
    local_sem,
    send_sem,
    recv_sem,
):
    n_group, n_page, n_tensor, slots, new_dev = dims
    n_y = n_group // CORES
    gi = lax.axis_index("group")
    z = lax.axis_index("page")
    x = lax.axis_index("tensor")
    y = lax.div(gi, CORES)
    core = lax.rem(gi, CORES)
    seqs = q.shape[0]
    kv_heads = key.shape[1] // HD
    share = q.shape[1] // HD // kv_heads
    rows = share * seqs
    cache_rows = slots * PAGE

    copies = []

    def fetch(src, dst):
        copy = pltpu.make_async_copy(src, dst, local_sem.at[len(copies)])
        copy.start()
        copies.append(copy)

    fetch(len_in, lens)
    fetch(pm_in, pm)
    fetch(tbl_in, tbl)
    fetch(q_in, q)
    fetch(ck_in, key.at[pl.ds(0, cache_rows)])
    fetch(nk_in, key.at[pl.ds(cache_rows, new_dev * PAGE)])
    fetch(cv_in, value.at[pl.ds(0, cache_rows)])
    fetch(nv_in, value.at[pl.ds(cache_rows, new_dev * PAGE)])
    fetch(w_in, weight)

    def along_group(d):
        return {"group": lax.rem(gi + d, n_group)}

    def along_sheet(d):
        other = lax.rem(z * CORES + core + d, n_page * CORES)
        return {"group": y * CORES + lax.rem(other, CORES), "page": lax.div(other, CORES)}

    def along_page(d):
        return {"page": lax.rem(z + d, n_page)}

    def along_y(d):
        return {"group": lax.rem(y + d, n_y) * CORES + core}

    def along_tensor(d):
        return {"tensor": lax.rem(x + d, n_tensor)}

    n_sheet = n_page * CORES
    place_b = z * CORES + core
    greeted = [along_group(d) for d in range(1, n_group)]
    for d in range(1, n_sheet):
        if d % CORES == 0:
            greeted.append(along_sheet(d))
    greeted_cross = [d for d in range(1, n_sheet) if d % CORES]
    greeted += [along_tensor(d) for d in range(1, n_tensor)]
    barrier = pltpu.get_barrier_semaphore()
    for peer in greeted:
        pl.semaphore_signal(barrier, inc=1, device_id=peer, device_id_type=MESH)
    for d in greeted_cross:
        pl.semaphore_signal(barrier, inc=1, device_id=along_sheet(d), device_id_type=MESH)

    def send(src, dst, peer, at):
        pltpu.make_async_remote_copy(
            src_ref=src,
            dst_ref=dst,
            send_sem=send_sem.at[at],
            recv_sem=recv_sem.at[at],
            device_id=peer,
            device_id_type=MESH,
        ).start()

    def received(ref, at):
        pltpu.make_async_copy(ref, ref, recv_sem.at[at]).wait()

    def left(ref, at):
        pltpu.make_async_copy(ref, ref, send_sem.at[at]).wait()

    for k in range(6):
        copies[k].wait()
    for half in range(kv_heads):
        heads = range(half * share, (half + 1) * share)
        stacked = jnp.concatenate([q[:, h * HD : (h + 1) * HD] for h in heads], axis=0)
        scores[half] = lax.dot_general(
            stacked,
            key[:, half * HD : (half + 1) * HD],
            NT,
            preferred_element_type=jnp.float32,
        )
    build_bias(tbl, pm, lens, tgt, bias, gi, z, n_page, slots, new_dev)
    for k in range(6, 8):
        copies[k].wait()

    def far_first(count):
        return sorted(range(1, count), key=lambda d: -min(d, count - d))

    def soften(half):
        block = 16
        for b in range(rows // block):
            s0 = b * block % seqs
            at = slice(b * block, (b + 1) * block)
            s = scores[half, at, :] * SCALE2 + bias[s0 : s0 + block, :]
            top = jnp.max(s, axis=1, keepdims=True)
            probs[half, at, :] = jnp.exp2(s - top).astype(jnp.bfloat16)
            tops[half, at, :] = jnp.broadcast_to(top, (block, LANES))

    def weigh(half, part, stat):
        count, own_rows = part.shape[0], part.shape[1]
        v = value[:, half * HD : (half + 1) * HD]
        wide = jnp.concatenate([v, jnp.ones_like(v)], axis=1)
        summed = jnp.dot(probs[half], wide, preferred_element_type=jnp.float32)
        shape = (own_rows, LANES)
        lane, row = lanes_of(shape), rows_of(shape)
        for k in range(count):
            at = slice(k * own_rows, (k + 1) * own_rows)
            part[k] = summed[at, :HD].astype(jnp.bfloat16)
            sums = jnp.where(lane == row + own_rows, summed[at, HD:], 0.0)
            picked = jnp.where(lane == row, tops[half, at, :], sums)
            stat[k] = jnp.sum(picked, axis=0, keepdims=True)

    def scatter(part, stat, got, gots, place, peer_of, at):
        count = part.shape[0]
        for d in far_first(count):
            owner = lax.rem(place + d, count)
            send(part.at[owner], got.at[d - 1], peer_of(d), at)
            send(stat.at[owner], gots.at[d - 1], peer_of(d), at + 1)

    def merge_scattered(part, stat, got, gots, mid, mids, place, at):
        count, own_rows = part.shape[0], part.shape[1]
        received(got, at)
        received(gots, at + 1)
        stats = [stat[place]] + [gots[d - 1] for d in range(1, count)]
        values = [part[place]] + [got[d - 1] for d in range(1, count)]
        highest, total, _, mixed = merge(stats, values, own_rows)
        mid[...] = mixed.astype(jnp.bfloat16)
        low = lanes_of((1, LANES)) < own_rows
        mids[...] = jnp.where(low, highest, pltpu.roll(total, own_rows, 1))

    def spread(mid, mids, gotm, gotms, peer_of, at):
        for d in far_first(gotm.shape[0] + 1):
            send(mid, gotm.at[d - 1], peer_of(d), at)
            send(mids, gotms.at[d - 1], peer_of(d), at + 1)

    def merge_spread(mid, mids, gotm, gotms, att, place, at):
        received(gotm, at)
        received(gotms, at + 1)
        others = range(gotm.shape[0])
        stats = [mids[...]] + [gotms[k] for k in others]
        values = [mid[...]] + [gotm[k] for k in others]
        _, _, total_column, mixed = merge(stats, values, mid.shape[0])
        att[place] = (mixed / total_column).astype(jnp.bfloat16)

    def gather(att, place, peer_of, at):
        for d in far_first(att.shape[0]):
            send(att.at[place], att.at[place], peer_of(d), at)

    soften(0)
    soften(1)
    weigh(0, part_a, stat_a)
    pl.semaphore_wait(barrier, len(greeted) + len(greeted_cross))
    scatter(part_a, stat_a, got_a, gots_a, gi, along_group, 0)
    weigh(1, part_b, stat_b)
    scatter(part_b, stat_b, got_b, gots_b, place_b, along_sheet, 2)
    merge_scattered(part_a, stat_a, got_a, gots_a, mid_a, mids_a, gi, 0)
    spread(mid_a, mids_a, gotm_a, gotms_a, along_page, 4)
    merge_scattered(part_b, stat_b, got_b, gots_b, mid_b, mids_b, place_b, 2)
    spread(mid_b, mids_b, gotm_b, gotms_b, along_y, 6)
    left(got_a, 0)
    left(gots_a, 1)
    left(got_b, 2)
    left(gots_b, 3)
    merge_spread(mid_a, mids_a, gotm_a, gotms_a, att_a, gi, 4)
    gather(att_a, gi, along_group, 8)
    merge_spread(mid_b, mids_b, gotm_b, gotms_b, att_b, place_b, 6)
    gather(att_b, place_b, along_sheet, 9)
    left(gotm_a, 4)
    left(gotms_a, 5)
    left(gotm_b, 6)
    left(gotms_b, 7)
    others_a = att_a.at[pl.ds(0, n_group - 1)]
    others_b = att_b.at[pl.ds(0, n_sheet - 1)]
    copies[8].wait()
    received(others_a, 8)
    received(others_b, 9)
    pieces = []
    for att in (att_a, att_b):
        flat = att[...].reshape(rows, HD)
        pieces += [flat[h * seqs : (h + 1) * seqs] for h in range(share)]
    features = jnp.concatenate(pieces, axis=1)
    last_out[...] = lax.dot_general(weight[...], features, NT, preferred_element_type=jnp.float32)
    width = out_ref.shape[0]

    def block_of(d):
        return last_out.at[pl.ds(pl.multiple_of(lax.rem(x + d, n_tensor) * width, width), width)]

    for d in far_first(n_tensor):
        send(block_of(d), last_in.at[d - 1], along_tensor(d), 10)
    left(others_a, 8)
    left(others_b, 9)
    received(last_in, 10)
    result = block_of(0)[...]
    for d in range(1, n_tensor):
        result = result + last_in[d - 1]
    out_ref[...] = result.astype(out_ref.dtype)
    left(last_in, 10)


def on_device(sizes, query, cache_keys, cache_values, new_keys, new_values, page_map, page_table, lengths, out_weight):
    n_group, n_page, n_tensor = sizes
    slots, page, width = cache_keys.shape
    new_dev = new_keys.shape[0]
    seqs = query.shape[0]
    tokens = (slots + new_dev) * page
    kv_heads = width // HD
    share = query.shape[1] // HD // kv_heads
    rows = share * seqs
    n_sheet = n_page * CORES
    n_y = n_group // CORES
    columns = out_weight.shape[1]
    rows_a, rows_b = rows // n_group, rows // n_sheet
    bf16, f32 = jnp.bfloat16, jnp.float32
    scratch = [
        pltpu.VMEM(query.shape, bf16),
        pltpu.VMEM((tokens, width), bf16),
        pltpu.VMEM((tokens, width), bf16),
        pltpu.VMEM((2, page_map.shape[0]), jnp.int32),
        pltpu.VMEM(page_table.shape, jnp.int32),
        pltpu.VMEM((1, seqs), jnp.int32),
        pltpu.VMEM((columns, out_weight.shape[0]), bf16),
        pltpu.VMEM((new_dev, LANES), jnp.int32),
        pltpu.VMEM((seqs, tokens), f32),
        pltpu.VMEM((kv_heads, rows, tokens), f32),
        pltpu.VMEM((kv_heads, rows, tokens), bf16),
        pltpu.VMEM((kv_heads, rows, LANES), f32),
        pltpu.VMEM((n_group, rows_a, HD), bf16),
        pltpu.VMEM((n_sheet, rows_b, HD), bf16),
        pltpu.VMEM((n_group, 1, LANES), f32),
        pltpu.VMEM((n_sheet, 1, LANES), f32),
        pltpu.VMEM((n_group - 1, rows_a, HD), bf16),
        pltpu.VMEM((n_sheet - 1, rows_b, HD), bf16),
        pltpu.VMEM((n_group - 1, 1, LANES), f32),
        pltpu.VMEM((n_sheet - 1, 1, LANES), f32),
        pltpu.VMEM((rows_a, HD), bf16),
        pltpu.VMEM((rows_b, HD), bf16),
        pltpu.VMEM((1, LANES), f32),
        pltpu.VMEM((1, LANES), f32),
        pltpu.VMEM((n_page - 1, rows_a, HD), bf16),
        pltpu.VMEM((n_y - 1, rows_b, HD), bf16),
        pltpu.VMEM((n_page - 1, 1, LANES), f32),
        pltpu.VMEM((n_y - 1, 1, LANES), f32),
        pltpu.VMEM((n_group, rows_a, HD), bf16),
        pltpu.VMEM((n_sheet, rows_b, HD), bf16),
        pltpu.VMEM((columns, seqs), f32),
        pltpu.VMEM((n_tensor - 1, columns // n_tensor, seqs), f32),
        pltpu.SemaphoreType.DMA((9,)),
        pltpu.SemaphoreType.DMA((11,)),
        pltpu.SemaphoreType.DMA((11,)),
    ]
    return pl.pallas_call(
        functools.partial(kernel, (n_group, n_page, n_tensor, slots, new_dev)),
        out_shape=pltpu.VMEM((columns // n_tensor, seqs), bf16),
        in_specs=[pl.BlockSpec(memory_space=pltpu.HBM)] * 9,
        out_specs=pl.BlockSpec(memory_space=pltpu.VMEM),
        scratch_shapes=scratch,
        compiler_params=pltpu.CompilerParams(
            collective_id=0, has_side_effects=True, vmem_limit_bytes=40 * 1024 * 1024
        ),
    )(*[pltpu.with_memory_space_constraint(a, pltpu.HBM) for a in (
        query,
        cache_keys.reshape(slots * page, width),
        cache_values.reshape(slots * page, width),
        new_keys.reshape(new_dev * page, width),
        new_values.reshape(new_dev * page, width),
        page_map.T,
        page_table,
        lengths.reshape(1, seqs),
        out_weight.T,
    )]).T


def solution(mesh):
    shards = ("group", "page")
    sizes = (mesh.shape["group"], mesh.shape["page"], mesh.shape["tensor"])
    placed = (
        P(None, "tensor"),
        P(shards, None, "tensor"),
        P(shards, None, "tensor"),
        P(shards, None, "tensor"),
        P(shards, None, "tensor"),
        P(),
        P(),
        P(),
        P("tensor", shards),
    )
    return jax.shard_map(
        functools.partial(on_device, sizes),
        mesh=mesh,
        in_specs=placed,
        out_specs=P(None, ("group", "page", "tensor")),
        check_vma=False,
    )
```

```python
import functools
import math

import jax
import jax.numpy as jnp
from jax import lax
from jax.experimental import pallas as pl
from jax.experimental.pallas import tpu as pltpu
from jax.sharding import PartitionSpec as P

HD = 128
PAGE = 16
LANES = 128
CORES = 2
MESH = pl.DeviceIdType.MESH
VERY_LOW = -1.0e30
PVS = 2
SCALE2 = HD**-0.5 * math.log2(math.e)
NT = (((1,), (1,)), ((), ()))


def lanes_of(shape):
    return lax.broadcasted_iota(jnp.int32, shape, len(shape) - 1)


def rows_of(shape):
    return lax.broadcasted_iota(jnp.int32, shape, len(shape) - 2)


def lane_sum(x):
    return jnp.sum(x.astype(jnp.float32), axis=1, keepdims=True).astype(jnp.int32)


def lane_or(words):
    low = lane_sum(words & 0xFFFF)
    high = lane_sum(lax.shift_right_logical(words, 16) & 0xFFFF)
    return low, high


def build_bias(tbl, pm, lens, tgt, bias, gi, z, n_page, slots, new_dev):
    seqs, pages = tbl.shape
    total = pm.shape[1]
    shard = gi * n_page + z
    base = shard * slots
    eye = rows_of((seqs, seqs)) == lanes_of((seqs, seqs))
    length = lane_sum(jnp.where(eye, lens[...], 0))
    used = (length + (PAGE - 1)) >> 4
    fill = length - (used - 1) * PAGE
    target = pm[0:1, :]
    slot = pm[1:2, :]
    number = lanes_of((1, total))
    sheet = (number // new_dev) % n_page
    valid = (target == gi) & (sheet == z)
    off = shard * new_dev
    own = jnp.where(
        lanes_of((new_dev, total)) == rows_of((new_dev, total)) + off,
        (target * n_page + z) * slots + slot,
        0,
    )
    tgt[...] = jnp.broadcast_to(lane_sum(own), tgt.shape)
    stale = []
    for w in range(slots // 16):
        hit = valid & ((slot >> 4) == w)
        stale.append(lane_sum(jnp.where(hit, jnp.int32(1) << (slot & 15), 0)))
    shape = (seqs, LANES)
    used_b = jnp.broadcast_to(used, shape)
    words = [jnp.zeros(shape, jnp.int32) for _ in range(slots // 32)]
    fresh = jnp.zeros(shape, jnp.int16)
    last = jnp.zeros(shape, jnp.int32)
    marks = [jnp.broadcast_to(tgt[k : k + 1, :], shape) for k in range(new_dev)]
    narrow_marks = [m.astype(jnp.int16) for m in marks]
    narrow_bits = [jnp.int16((1 << k) if k < 15 else -(1 << 15)) for k in range(new_dev)]
    for c in range(pages // LANES):
        entry = tbl[:, c * LANES : (c + 1) * LANES]
        j = lanes_of(shape) + c * LANES
        last = last + jnp.where(j == used_b - 1, entry, 0)
        entry = jnp.where(j < used_b, entry, -1)
        local = entry - base
        high = local >> 5
        bit = jnp.int32(1) << (local & 31)
        for w in range(slots // 32):
            words[w] = words[w] | jnp.where(high == w, bit, 0)
        narrow = entry.astype(jnp.int16)
        for k in range(new_dev):
            fresh = fresh | jnp.where(narrow == narrow_marks[k], narrow_bits[k], jnp.int16(0))
    last_b = jnp.broadcast_to(lane_sum(last), shape)
    fill_b = jnp.broadcast_to(fill, shape)
    owned = []
    for w in range(slots // 32):
        owned.extend(lane_or(words[w]))
    fresh_b = jnp.broadcast_to(lane_sum(fresh.astype(jnp.int32) & 0xFFFF), shape)
    last_fresh = jnp.zeros(shape, jnp.int32)
    for k in range(new_dev):
        last_fresh = last_fresh | jnp.where(last_b == marks[k], 1 << k, 0)
    lane = lanes_of(shape)
    tail_end = (last_b - base) * PAGE + PAGE
    tail_start = tail_end - PAGE + fill_b
    per_tile = LANES // PAGE
    for w in range(slots // 16):
        word = jnp.broadcast_to(owned[w] & ~stale[w], shape)
        for half in range(16 // per_tile):
            c = w * (16 // per_tile) + half
            token = lane + c * LANES
            here = (lax.shift_right_logical(word, (lane >> 4) + half * per_tile) & 1) == 1
            here = here & ((token < tail_start) | (token >= tail_end))
            bias[:, c * LANES : (c + 1) * LANES] = jnp.where(here, 0.0, VERY_LOW)
    first = slots * PAGE
    for c in range(new_dev // per_tile):
        shift = (lane >> 4) + c * per_tile
        here = (lax.shift_right_logical(fresh_b, shift) & 1) == 1
        ends = (lax.shift_right_logical(last_fresh, shift) & 1) == 1
        here = here & ~(ends & ((lane & 15) >= fill_b))
        bias[:, first + c * LANES : first + (c + 1) * LANES] = jnp.where(here, 0.0, VERY_LOW)


def merge(stat_rows, values, rows):
    count = len(stat_rows)
    pad = [jnp.zeros((-count % 8, LANES), jnp.float32)] if count % 8 else []
    stats = jnp.concatenate(stat_rows + pad, axis=0)
    real = rows_of(stats.shape) < count
    highest = jnp.max(jnp.where(real, stats, -jnp.inf), axis=0, keepdims=True)
    in_max = lanes_of(stats.shape) < rows
    factor = jnp.where(real & in_max, jnp.exp2(jnp.where(in_max, stats - highest, 0.0)), 0.0)
    sums = pltpu.roll(stats, LANES - rows, 1)
    total = jnp.sum(factor * jnp.where(in_max, sums, 0.0), axis=0, keepdims=True)
    square = jnp.concatenate(
        [factor, jnp.broadcast_to(total, (8, LANES)), jnp.zeros((LANES - 8 - stats.shape[0], LANES), jnp.float32)],
        axis=0,
    )
    across = square.T
    mixed = across[:rows, 0:1] * values[0].astype(jnp.float32)
    for k in range(1, count):
        mixed = mixed + across[:rows, k : k + 1] * values[k].astype(jnp.float32)
    total_column = across[:rows, stats.shape[0] : stats.shape[0] + 1]
    return highest, total, total_column, mixed


def kernel(
    dims,
    q_in,
    ck_in,
    cv_in,
    nk_in,
    nv_in,
    pm_in,
    tbl_in,
    len_in,
    w_in,
    out_ref,
    q,
    key,
    value,
    pm,
    tbl,
    lens,
    weight,
    tgt,
    bias,
    scores,
    probs,
    tops,
    part_a,
    part_b,
    stat_a,
    stat_b,
    got_a,
    got_b,
    gots_a,
    gots_b,
    mid_a,
    mid_b,
    mids_a,
    mids_b,
    gotm_a,
    gotm_b,
    gotms_a,
    gotms_b,
    att_a,
    att_b,
    last_out,
    last_in,
    local_sem,
    send_sem,
    recv_sem,
):
    n_group, n_page, n_tensor, slots, new_dev = dims
    n_y = n_group // CORES
    gi = lax.axis_index("group")
    z = lax.axis_index("page")
    x = lax.axis_index("tensor")
    y = lax.div(gi, CORES)
    core = lax.rem(gi, CORES)
    seqs = q.shape[0]
    kv_heads = key.shape[1] // HD
    share = q.shape[1] // HD // kv_heads
    rows = share * seqs
    cache_rows = slots * PAGE

    copies = []

    def fetch(src, dst):
        copy = pltpu.make_async_copy(src, dst, local_sem.at[len(copies)])
        copy.start()
        copies.append(copy)

    fetch(len_in, lens)
    fetch(pm_in, pm)
    fetch(tbl_in, tbl)
    fetch(q_in, q)
    fetch(ck_in, key.at[pl.ds(0, cache_rows)])
    fetch(nk_in, key.at[pl.ds(cache_rows, new_dev * PAGE)])
    fetch(cv_in, value.at[pl.ds(0, cache_rows)])
    fetch(nv_in, value.at[pl.ds(cache_rows, new_dev * PAGE)])
    fetch(w_in, weight)

    def along_group(d):
        return {"group": lax.rem(gi + d, n_group)}

    def along_sheet(d):
        other = lax.rem(z * CORES + core + d, n_page * CORES)
        return {"group": y * CORES + lax.rem(other, CORES), "page": lax.div(other, CORES)}

    def along_page(d):
        return {"page": lax.rem(z + d, n_page)}

    def along_y(d):
        return {"group": lax.rem(y + d, n_y) * CORES + core}

    def along_tensor(d):
        return {"tensor": lax.rem(x + d, n_tensor)}

    n_sheet = n_page * CORES
    place_b = z * CORES + core
    barrier = pltpu.get_barrier_semaphore()

    def other_core(place, d, count):
        return lax.rem(place + d, count) * CORES + 1 - core

    peers = []
    for d in range(1, n_page):
        hops = min(d, n_page - d)
        peers.append((hops, along_page(d)))
        peers.append((hops, {"group": y * CORES + 1 - core, "page": lax.rem(z + d, n_page)}))
    for d in range(1, n_y):
        hops = min(d, n_y - d)
        peers.append((hops, along_y(d)))
        peers.append((hops, {"group": other_core(y, d, n_y)}))
    peers += [(min(d, n_tensor - d), along_tensor(d)) for d in range(1, n_tensor)]
    peers.append((0, {"group": y * CORES + 1 - core}))
    for _, peer in sorted(peers, key=lambda p: -p[0]):
        pl.semaphore_signal(barrier, inc=1, device_id=peer, device_id_type=MESH)

    def send(src, dst, peer, at):
        pltpu.make_async_remote_copy(
            src_ref=src,
            dst_ref=dst,
            send_sem=send_sem.at[at],
            recv_sem=recv_sem.at[at],
            device_id=peer,
            device_id_type=MESH,
        ).start()

    def received(ref, at):
        pltpu.make_async_copy(ref, ref, recv_sem.at[at]).wait()

    def left(ref, at):
        pltpu.make_async_copy(ref, ref, send_sem.at[at]).wait()

    for k in range(3):
        copies[k].wait()
    build_bias(tbl, pm, lens, tgt, bias, gi, z, n_page, slots, new_dev)
    for k in range(3, 6):
        copies[k].wait()

    def score(half):
        heads = range(half * share, (half + 1) * share)
        stacked = jnp.concatenate([q[:, h * HD : (h + 1) * HD] for h in heads], axis=0)
        s = lax.dot_general(
            stacked,
            key[:, half * HD : (half + 1) * HD],
            NT,
            preferred_element_type=jnp.float32,
        )
        for h in range(share):
            at = slice(h * seqs, (h + 1) * seqs)
            scores[half, at, :] = s[at, :] * SCALE2 + bias[...]

    def far_first(count):
        return sorted(range(1, count), key=lambda d: -min(d, count - d))

    def soften(half):
        block = 16
        for b in range(rows // block):
            at = slice(b * block, (b + 1) * block)
            s = scores[half, at, :]
            top = jnp.max(s, axis=1, keepdims=True)
            probs[half, at, :] = jnp.exp2(s - top).astype(jnp.bfloat16)
            tops[half, at, :] = jnp.broadcast_to(top, (block, LANES))

    def weigh(half, part, stat):
        count, own_rows = part.shape[0], part.shape[1]
        v = value[:, half * HD : (half + 1) * HD]
        wide = jnp.concatenate([v, jnp.ones_like(v)], axis=1)
        summed = jnp.concatenate(
            [
                jnp.dot(probs[half, i * rows // PVS : (i + 1) * rows // PVS, :], wide, preferred_element_type=jnp.float32)
                for i in range(PVS)
            ],
            axis=0,
        )
        shape = (own_rows, LANES)
        lane, row = lanes_of(shape), rows_of(shape)
        for k in range(count):
            at = slice(k * own_rows, (k + 1) * own_rows)
            part[k] = summed[at, :HD].astype(jnp.bfloat16)
            sums = jnp.where(lane == row + own_rows, summed[at, HD:], 0.0)
            picked = jnp.where(lane == row, tops[half, at, :], sums)
            stat[k] = jnp.sum(picked, axis=0, keepdims=True)

    def near_root(count):
        return sorted(range(count), key=lambda k: min(k, count - k))

    def scatter(part, stat, got, gots, place, peer_of, at):
        count = part.shape[0]
        for d in far_first(count):
            owner = lax.rem(place + d, count)
            send(part.at[owner], got.at[d - 1], peer_of(d), at)
            send(stat.at[owner], gots.at[d - 1], peer_of(d), at + 1)

    def merge_scattered(part, stat, got, gots, mid, mids, place, at):
        count, own_rows = part.shape[0], part.shape[1]
        received(got, at)
        received(gots, at + 1)
        stats = [stat[place]] + [gots[d - 1] for d in range(1, count)]
        values = [part[place]] + [got[d - 1] for d in range(1, count)]
        highest, total, _, mixed = merge(stats, values, own_rows)
        mid[...] = mixed.astype(jnp.bfloat16)
        low = lanes_of((1, LANES)) < own_rows
        mids[...] = jnp.where(low, highest, pltpu.roll(total, own_rows, 1))

    def spread(mid, mids, gotm, gotms, place, peer_at, at):
        count = gotm.shape[0] + 1
        for k in near_root(count):

            @pl.when(place != k)
            def _():
                slot = lax.rem(k - place + count, count) - 1
                send(mid, gotm.at[slot], peer_at(k), at)
                send(mids, gotms.at[slot], peer_at(k), at + 1)

    def merge_spread(mid, mids, gotm, gotms, att, place, at):
        received(gotm, at)
        received(gotms, at + 1)
        others = range(gotm.shape[0])
        stats = [mids[...]] + [gotms[k] for k in others]
        values = [mid[...]] + [gotm[k] for k in others]
        _, _, total_column, mixed = merge(stats, values, mid.shape[0])
        att[place] = (mixed / total_column).astype(jnp.bfloat16)

    def gather(att, place, peer_at, at):
        count = att.shape[0]
        for k in near_root(count // CORES):
            for c in (1, 0):
                spot = k * CORES + c

                @pl.when(place != spot)
                def _():
                    send(att.at[place], att.at[place], peer_at(k, c), at)

    score(1)
    soften(1)
    for k in range(6, 8):
        copies[k].wait()
    weigh(1, part_b, stat_b)
    pl.semaphore_wait(barrier, len(peers))
    scatter(part_b, stat_b, got_b, gots_b, place_b, along_sheet, 2)
    score(0)
    soften(0)
    weigh(0, part_a, stat_a)
    scatter(part_a, stat_a, got_a, gots_a, gi, along_group, 0)
    merge_scattered(part_b, stat_b, got_b, gots_b, mid_b, mids_b, place_b, 2)
    spread(mid_b, mids_b, gotm_b, gotms_b, y, lambda k: {"group": k * CORES + core}, 6)
    merge_scattered(part_a, stat_a, got_a, gots_a, mid_a, mids_a, gi, 0)
    spread(mid_a, mids_a, gotm_a, gotms_a, z, lambda k: {"page": k}, 4)
    left(got_a, 0)
    left(gots_a, 1)
    left(got_b, 2)
    left(gots_b, 3)
    merge_spread(mid_b, mids_b, gotm_b, gotms_b, att_b, place_b, 6)
    gather(att_b, place_b, lambda k, c: {"group": y * CORES + c, "page": k}, 9)
    merge_spread(mid_a, mids_a, gotm_a, gotms_a, att_a, gi, 4)
    gather(att_a, gi, lambda k, c: {"group": k * CORES + c}, 8)
    left(gotm_a, 4)
    left(gotms_a, 5)
    left(gotm_b, 6)
    left(gotms_b, 7)
    others_a = att_a.at[pl.ds(0, n_group - 1)]
    others_b = att_b.at[pl.ds(0, n_sheet - 1)]
    copies[8].wait()
    received(others_a, 8)
    received(others_b, 9)
    pieces = []
    for att in (att_a, att_b):
        flat = att[...].reshape(rows, HD)
        pieces += [flat[h * seqs : (h + 1) * seqs] for h in range(share)]
    features = jnp.concatenate(pieces, axis=1)
    last_out[...] = lax.dot_general(weight[...], features, NT, preferred_element_type=jnp.float32)
    width = out_ref.shape[0]

    def block_of(d):
        return last_out.at[pl.ds(pl.multiple_of(lax.rem(x + d, n_tensor) * width, width), width)]

    for d in far_first(n_tensor):
        send(block_of(d), last_in.at[d - 1], along_tensor(d), 10)
    left(others_a, 8)
    left(others_b, 9)
    received(last_in, 10)
    result = block_of(0)[...]
    for d in range(1, n_tensor):
        result = result + last_in[d - 1]
    out_ref[...] = result.astype(out_ref.dtype)
    left(last_in, 10)


def on_device(sizes, query, cache_keys, cache_values, new_keys, new_values, page_map, page_table, lengths, out_weight):
    n_group, n_page, n_tensor = sizes
    slots, page, width = cache_keys.shape
    new_dev = new_keys.shape[0]
    seqs = query.shape[0]
    tokens = (slots + new_dev) * page
    kv_heads = width // HD
    share = query.shape[1] // HD // kv_heads
    rows = share * seqs
    n_sheet = n_page * CORES
    n_y = n_group // CORES
    columns = out_weight.shape[1]
    rows_a, rows_b = rows // n_group, rows // n_sheet
    bf16, f32 = jnp.bfloat16, jnp.float32
    scratch = [
        pltpu.VMEM(query.shape, bf16),
        pltpu.VMEM((tokens, width), bf16),
        pltpu.VMEM((tokens, width), bf16),
        pltpu.VMEM((2, page_map.shape[0]), jnp.int32),
        pltpu.VMEM(page_table.shape, jnp.int32),
        pltpu.VMEM((1, seqs), jnp.int32),
        pltpu.VMEM((columns, out_weight.shape[0]), bf16),
        pltpu.VMEM((new_dev, LANES), jnp.int32),
        pltpu.VMEM((seqs, tokens), f32),
        pltpu.VMEM((kv_heads, rows, tokens), f32),
        pltpu.VMEM((kv_heads, rows, tokens), bf16),
        pltpu.VMEM((kv_heads, rows, LANES), f32),
        pltpu.VMEM((n_group, rows_a, HD), bf16),
        pltpu.VMEM((n_sheet, rows_b, HD), bf16),
        pltpu.VMEM((n_group, 1, LANES), f32),
        pltpu.VMEM((n_sheet, 1, LANES), f32),
        pltpu.VMEM((n_group - 1, rows_a, HD), bf16),
        pltpu.VMEM((n_sheet - 1, rows_b, HD), bf16),
        pltpu.VMEM((n_group - 1, 1, LANES), f32),
        pltpu.VMEM((n_sheet - 1, 1, LANES), f32),
        pltpu.VMEM((rows_a, HD), bf16),
        pltpu.VMEM((rows_b, HD), bf16),
        pltpu.VMEM((1, LANES), f32),
        pltpu.VMEM((1, LANES), f32),
        pltpu.VMEM((n_page - 1, rows_a, HD), bf16),
        pltpu.VMEM((n_y - 1, rows_b, HD), bf16),
        pltpu.VMEM((n_page - 1, 1, LANES), f32),
        pltpu.VMEM((n_y - 1, 1, LANES), f32),
        pltpu.VMEM((n_group, rows_a, HD), bf16),
        pltpu.VMEM((n_sheet, rows_b, HD), bf16),
        pltpu.VMEM((columns, seqs), f32),
        pltpu.VMEM((n_tensor - 1, columns // n_tensor, seqs), f32),
        pltpu.SemaphoreType.DMA((9,)),
        pltpu.SemaphoreType.DMA((11,)),
        pltpu.SemaphoreType.DMA((11,)),
    ]
    return pl.pallas_call(
        functools.partial(kernel, (n_group, n_page, n_tensor, slots, new_dev)),
        out_shape=pltpu.VMEM((columns // n_tensor, seqs), bf16),
        in_specs=[pl.BlockSpec(memory_space=pltpu.HBM)] * 9,
        out_specs=pl.BlockSpec(memory_space=pltpu.VMEM),
        scratch_shapes=scratch,
        compiler_params=pltpu.CompilerParams(
            collective_id=0, has_side_effects=True, vmem_limit_bytes=40 * 1024 * 1024
        ),
    )(*[pltpu.with_memory_space_constraint(a, pltpu.HBM) for a in (
        query,
        cache_keys.reshape(slots * page, width),
        cache_values.reshape(slots * page, width),
        new_keys.reshape(new_dev * page, width),
        new_values.reshape(new_dev * page, width),
        page_map.T,
        page_table,
        lengths.reshape(1, seqs),
        out_weight.T,
    )]).T


def solution(mesh):
    shards = ("group", "page")
    sizes = (mesh.shape["group"], mesh.shape["page"], mesh.shape["tensor"])
    placed = (
        P(None, "tensor"),
        P(shards, None, "tensor"),
        P(shards, None, "tensor"),
        P(shards, None, "tensor"),
        P(shards, None, "tensor"),
        P(),
        P(),
        P(),
        P("tensor", shards),
    )
    return jax.shard_map(
        functools.partial(on_device, sizes),
        mesh=mesh,
        in_specs=placed,
        out_specs=P(None, ("group", "page", "tensor")),
        check_vma=False,
    )
```

```python
import functools
import math

import jax
import jax.numpy as jnp
from jax import lax
from jax.experimental import pallas as pl
from jax.experimental.pallas import tpu as pltpu
from jax.sharding import PartitionSpec as P

HD = 128
PAGE = 16
LANES = 128
CORES = 2
MESH = pl.DeviceIdType.MESH
VERY_LOW = -1.0e30
PVS = 2
SCALE2 = HD**-0.5 * math.log2(math.e)
NT = (((1,), (1,)), ((), ()))


def lanes_of(shape):
    return lax.broadcasted_iota(jnp.int32, shape, len(shape) - 1)


def rows_of(shape):
    return lax.broadcasted_iota(jnp.int32, shape, len(shape) - 2)


def lane_sum(x):
    return jnp.sum(x.astype(jnp.float32), axis=1, keepdims=True).astype(jnp.int32)


def lane_or(words):
    low = lane_sum(words & 0xFFFF)
    high = lane_sum(lax.shift_right_logical(words, 16) & 0xFFFF)
    return low, high


def build_bias(tbl, pm, lens, tgt, bias, gi, z, n_page, slots, new_dev):
    seqs, pages = tbl.shape
    total = pm.shape[1]
    shard = gi * n_page + z
    base = shard * slots
    eye = rows_of((seqs, seqs)) == lanes_of((seqs, seqs))
    length = lane_sum(jnp.where(eye, lens[...], 0))
    used = (length + (PAGE - 1)) >> 4
    fill = length - (used - 1) * PAGE
    target = pm[0:1, :]
    slot = pm[1:2, :]
    number = lanes_of((1, total))
    sheet = (number // new_dev) % n_page
    valid = (target == gi) & (sheet == z)
    off = shard * new_dev
    own = jnp.where(
        lanes_of((new_dev, total)) == rows_of((new_dev, total)) + off,
        (target * n_page + z) * slots + slot,
        0,
    )
    tgt[...] = jnp.broadcast_to(lane_sum(own), tgt.shape)
    stale = []
    for w in range(slots // 16):
        hit = valid & ((slot >> 4) == w)
        stale.append(lane_sum(jnp.where(hit, jnp.int32(1) << (slot & 15), 0)))
    shape = (seqs, LANES)
    used_b = jnp.broadcast_to(used, shape)
    words = [jnp.zeros(shape, jnp.int32) for _ in range(slots // 32)]
    fresh = jnp.zeros(shape, jnp.int16)
    last = jnp.zeros(shape, jnp.int32)
    marks = [jnp.broadcast_to(tgt[k : k + 1, :], shape) for k in range(new_dev)]
    narrow_marks = [m.astype(jnp.int16) for m in marks]
    narrow_bits = [jnp.int16((1 << k) if k < 15 else -(1 << 15)) for k in range(new_dev)]
    for c in range(pages // LANES):
        entry = tbl[:, c * LANES : (c + 1) * LANES]
        j = lanes_of(shape) + c * LANES
        last = last + jnp.where(j == used_b - 1, entry, 0)
        entry = jnp.where(j < used_b, entry, -1)
        local = entry - base
        high = local >> 5
        bit = jnp.int32(1) << (local & 31)
        for w in range(slots // 32):
            words[w] = words[w] | jnp.where(high == w, bit, 0)
        narrow = entry.astype(jnp.int16)
        for k in range(new_dev):
            fresh = fresh | jnp.where(narrow == narrow_marks[k], narrow_bits[k], jnp.int16(0))
    last_b = jnp.broadcast_to(lane_sum(last), shape)
    fill_b = jnp.broadcast_to(fill, shape)
    owned = []
    for w in range(slots // 32):
        owned.extend(lane_or(words[w]))
    fresh_b = jnp.broadcast_to(lane_sum(fresh.astype(jnp.int32) & 0xFFFF), shape)
    last_fresh = jnp.zeros(shape, jnp.int32)
    for k in range(new_dev):
        last_fresh = last_fresh | jnp.where(last_b == marks[k], 1 << k, 0)
    lane = lanes_of(shape)
    tail_end = (last_b - base) * PAGE + PAGE
    tail_start = tail_end - PAGE + fill_b
    per_tile = LANES // PAGE
    for w in range(slots // 16):
        word = jnp.broadcast_to(owned[w] & ~stale[w], shape)
        for half in range(16 // per_tile):
            c = w * (16 // per_tile) + half
            token = lane + c * LANES
            here = (lax.shift_right_logical(word, (lane >> 4) + half * per_tile) & 1) == 1
            here = here & ((token < tail_start) | (token >= tail_end))
            bias[:, c * LANES : (c + 1) * LANES] = jnp.where(here, 0.0, VERY_LOW)
    first = slots * PAGE
    for c in range(new_dev // per_tile):
        shift = (lane >> 4) + c * per_tile
        here = (lax.shift_right_logical(fresh_b, shift) & 1) == 1
        ends = (lax.shift_right_logical(last_fresh, shift) & 1) == 1
        here = here & ~(ends & ((lane & 15) >= fill_b))
        bias[:, first + c * LANES : first + (c + 1) * LANES] = jnp.where(here, 0.0, VERY_LOW)


def merge(stat_rows, values, rows):
    count = len(stat_rows)
    pad = [jnp.zeros((-count % 8, LANES), jnp.float32)] if count % 8 else []
    stats = jnp.concatenate(stat_rows + pad, axis=0)
    real = rows_of(stats.shape) < count
    highest = jnp.max(jnp.where(real, stats, -jnp.inf), axis=0, keepdims=True)
    in_max = lanes_of(stats.shape) < rows
    factor = jnp.where(real & in_max, jnp.exp2(jnp.where(in_max, stats - highest, 0.0)), 0.0)
    sums = pltpu.roll(stats, LANES - rows, 1)
    total = jnp.sum(factor * jnp.where(in_max, sums, 0.0), axis=0, keepdims=True)
    square = jnp.concatenate(
        [factor, jnp.broadcast_to(total, (8, LANES)), jnp.zeros((LANES - 8 - stats.shape[0], LANES), jnp.float32)],
        axis=0,
    )
    across = square.T
    mixed = across[:rows, 0:1] * values[0].astype(jnp.float32)
    for k in range(1, count):
        mixed = mixed + across[:rows, k : k + 1] * values[k].astype(jnp.float32)
    total_column = across[:rows, stats.shape[0] : stats.shape[0] + 1]
    return highest, total, total_column, mixed


def kernel(
    dims,
    q_in,
    ck_in,
    cv_in,
    nk_in,
    nv_in,
    pm_in,
    tbl_in,
    len_in,
    w_in,
    out_ref,
    q,
    key,
    value,
    pm,
    tbl,
    lens,
    weight,
    tgt,
    bias,
    scores,
    probs,
    tops,
    part_a,
    part_b,
    stat_a,
    stat_b,
    got_a,
    got_b,
    gots_a,
    gots_b,
    mid_a,
    mid_b,
    mids_a,
    mids_b,
    gotm_a,
    gotm_b,
    gotms_a,
    gotms_b,
    att_a,
    att_b,
    last_out,
    last_in,
    local_sem,
    send_sem,
    recv_sem,
):
    n_group, n_page, n_tensor, slots, new_dev = dims
    n_y = n_group // CORES
    gi = lax.axis_index("group")
    z = lax.axis_index("page")
    x = lax.axis_index("tensor")
    y = lax.div(gi, CORES)
    core = lax.rem(gi, CORES)
    seqs = q.shape[0]
    kv_heads = key.shape[1] // HD
    share = q.shape[1] // HD // kv_heads
    rows = share * seqs
    cache_rows = slots * PAGE

    copies = []

    def fetch(src, dst):
        copy = pltpu.make_async_copy(src, dst, local_sem.at[len(copies)])
        copy.start()
        copies.append(copy)

    fetch(len_in, lens)
    fetch(pm_in, pm)
    fetch(tbl_in, tbl)
    fetch(q_in, q)
    fetch(ck_in, key.at[pl.ds(0, cache_rows)])
    fetch(nk_in, key.at[pl.ds(cache_rows, new_dev * PAGE)])
    fetch(cv_in, value.at[pl.ds(0, cache_rows)])
    fetch(nv_in, value.at[pl.ds(cache_rows, new_dev * PAGE)])
    fetch(w_in, weight)

    def along_group(d):
        return {"group": lax.rem(gi + d, n_group)}

    def along_sheet(d):
        other = lax.rem(z * CORES + core + d, n_page * CORES)
        return {"group": y * CORES + lax.rem(other, CORES), "page": lax.div(other, CORES)}

    def along_page(d):
        return {"page": lax.rem(z + d, n_page)}

    def along_y(d):
        return {"group": lax.rem(y + d, n_y) * CORES + core}

    def along_tensor(d):
        return {"tensor": lax.rem(x + d, n_tensor)}

    n_sheet = n_page * CORES
    place_b = z * CORES + core
    barrier = pltpu.get_barrier_semaphore()

    def other_core(place, d, count):
        return lax.rem(place + d, count) * CORES + 1 - core

    peers = []
    for d in range(1, n_page):
        hops = min(d, n_page - d)
        peers.append((hops, along_page(d)))
        peers.append((hops, {"group": y * CORES + 1 - core, "page": lax.rem(z + d, n_page)}))
    for d in range(1, n_y):
        hops = min(d, n_y - d)
        peers.append((hops, along_y(d)))
        peers.append((hops, {"group": other_core(y, d, n_y)}))
    peers += [(min(d, n_tensor - d), along_tensor(d)) for d in range(1, n_tensor)]
    peers.append((0, {"group": y * CORES + 1 - core}))
    for _, peer in sorted(peers, key=lambda p: -p[0]):
        pl.semaphore_signal(barrier, inc=1, device_id=peer, device_id_type=MESH)

    def send(src, dst, peer, at):
        pltpu.make_async_remote_copy(
            src_ref=src,
            dst_ref=dst,
            send_sem=send_sem.at[at],
            recv_sem=recv_sem.at[at],
            device_id=peer,
            device_id_type=MESH,
        ).start()

    def received(ref, at):
        pltpu.make_async_copy(ref, ref, recv_sem.at[at]).wait()

    def left(ref, at):
        pltpu.make_async_copy(ref, ref, send_sem.at[at]).wait()

    for k in range(3):
        copies[k].wait()
    build_bias(tbl, pm, lens, tgt, bias, gi, z, n_page, slots, new_dev)
    for k in range(3, 6):
        copies[k].wait()

    def score(half):
        heads = range(half * share, (half + 1) * share)
        stacked = jnp.concatenate([q[:, h * HD : (h + 1) * HD] for h in heads], axis=0)
        s = lax.dot_general(
            stacked,
            key[:, half * HD : (half + 1) * HD],
            NT,
            preferred_element_type=jnp.float32,
        )
        for h in range(share):
            at = slice(h * seqs, (h + 1) * seqs)
            scores[half, at, :] = s[at, :] * SCALE2 + bias[...]

    def far_first(count):
        return sorted(range(1, count), key=lambda d: -min(d, count - d))

    def soften(half):
        block = 16
        for b in range(rows // block):
            at = slice(b * block, (b + 1) * block)
            s = scores[half, at, :]
            top = jnp.max(s, axis=1, keepdims=True)
            probs[half, at, :] = jnp.exp2(s - top).astype(jnp.bfloat16)
            tops[half, at, :] = jnp.broadcast_to(top, (block, LANES))

    def weigh(half, part, stat):
        count, own_rows = part.shape[0], part.shape[1]
        v = value[:, half * HD : (half + 1) * HD]
        wide = jnp.concatenate([v, jnp.ones_like(v)], axis=1)
        summed = jnp.concatenate(
            [
                jnp.dot(probs[half, i * rows // PVS : (i + 1) * rows // PVS, :], wide, preferred_element_type=jnp.float32)
                for i in range(PVS)
            ],
            axis=0,
        )
        shape = (own_rows, LANES)
        lane, row = lanes_of(shape), rows_of(shape)
        for k in range(count):
            at = slice(k * own_rows, (k + 1) * own_rows)
            part[k] = summed[at, :HD].astype(jnp.bfloat16)
            sums = jnp.where(lane == row + own_rows, summed[at, HD:], 0.0)
            picked = jnp.where(lane == row, tops[half, at, :], sums)
            stat[k] = jnp.sum(picked, axis=0, keepdims=True)

    def near_root(count):
        return sorted(range(count), key=lambda k: min(k, count - k))

    def scatter(part, stat, got, gots, place, peer_at, at):
        count = part.shape[0]
        for k in reversed(near_root(count // CORES)):
            for c in range(CORES):
                spot = k * CORES + c

                @pl.when(place != spot)
                def _():
                    slot = lax.rem(spot - place + count, count) - 1
                    send(part.at[spot], got.at[slot], peer_at(k, c), at)
                    send(stat.at[spot], gots.at[slot], peer_at(k, c), at + 1)

    def merge_scattered(part, stat, got, gots, mid, mids, place, at):
        count, own_rows = part.shape[0], part.shape[1]
        received(got, at)
        received(gots, at + 1)
        stats = [stat[place]] + [gots[d - 1] for d in range(1, count)]
        values = [part[place]] + [got[d - 1] for d in range(1, count)]
        highest, total, _, mixed = merge(stats, values, own_rows)
        mid[...] = mixed.astype(jnp.bfloat16)
        low = lanes_of((1, LANES)) < own_rows
        mids[...] = jnp.where(low, highest, pltpu.roll(total, own_rows, 1))

    def spread(mid, mids, gotm, gotms, place, peer_at, at):
        count = gotm.shape[0] + 1
        for k in near_root(count):

            @pl.when(place != k)
            def _():
                slot = lax.rem(k - place + count, count) - 1
                send(mid, gotm.at[slot], peer_at(k), at)
                send(mids, gotms.at[slot], peer_at(k), at + 1)

    def merge_spread(mid, mids, gotm, gotms, att, place, at):
        received(gotm, at)
        received(gotms, at + 1)
        others = range(gotm.shape[0])
        stats = [mids[...]] + [gotms[k] for k in others]
        values = [mid[...]] + [gotm[k] for k in others]
        _, _, total_column, mixed = merge(stats, values, mid.shape[0])
        att[place] = (mixed / total_column).astype(jnp.bfloat16)

    def gather(att, place, peer_at, at):
        count = att.shape[0]
        for k in near_root(count // CORES):
            for c in (1, 0):
                spot = k * CORES + c

                @pl.when(place != spot)
                def _():
                    send(att.at[place], att.at[place], peer_at(k, c), at)

    score(1)
    soften(1)
    for k in range(6, 8):
        copies[k].wait()
    weigh(1, part_b, stat_b)
    pl.semaphore_wait(barrier, len(peers))
    scatter(part_b, stat_b, got_b, gots_b, place_b, lambda k, c: {"group": y * CORES + c, "page": k}, 2)
    score(0)
    soften(0)
    weigh(0, part_a, stat_a)
    scatter(part_a, stat_a, got_a, gots_a, gi, lambda k, c: {"group": k * CORES + c}, 0)
    merge_scattered(part_b, stat_b, got_b, gots_b, mid_b, mids_b, place_b, 2)
    spread(mid_b, mids_b, gotm_b, gotms_b, y, lambda k: {"group": k * CORES + core}, 6)
    merge_scattered(part_a, stat_a, got_a, gots_a, mid_a, mids_a, gi, 0)
    spread(mid_a, mids_a, gotm_a, gotms_a, z, lambda k: {"page": k}, 4)
    left(got_a, 0)
    left(gots_a, 1)
    left(got_b, 2)
    left(gots_b, 3)
    merge_spread(mid_b, mids_b, gotm_b, gotms_b, att_b, place_b, 6)
    gather(att_b, place_b, lambda k, c: {"group": y * CORES + c, "page": k}, 9)
    merge_spread(mid_a, mids_a, gotm_a, gotms_a, att_a, gi, 4)
    gather(att_a, gi, lambda k, c: {"group": k * CORES + c}, 8)
    left(gotm_a, 4)
    left(gotms_a, 5)
    left(gotm_b, 6)
    left(gotms_b, 7)
    others_a = att_a.at[pl.ds(0, n_group - 1)]
    others_b = att_b.at[pl.ds(0, n_sheet - 1)]
    copies[8].wait()
    received(others_a, 8)
    received(others_b, 9)
    pieces = []
    for att in (att_a, att_b):
        flat = att[...].reshape(rows, HD)
        pieces += [flat[h * seqs : (h + 1) * seqs] for h in range(share)]
    features = jnp.concatenate(pieces, axis=1)
    last_out[...] = lax.dot_general(weight[...], features, NT, preferred_element_type=jnp.float32)
    width = out_ref.shape[0]

    def block_of(d):
        return last_out.at[pl.ds(pl.multiple_of(lax.rem(x + d, n_tensor) * width, width), width)]

    for d in far_first(n_tensor):
        send(block_of(d), last_in.at[d - 1], along_tensor(d), 10)
    left(others_a, 8)
    left(others_b, 9)
    received(last_in, 10)
    result = block_of(0)[...]
    for d in range(1, n_tensor):
        result = result + last_in[d - 1]
    out_ref[...] = result.astype(out_ref.dtype)
    left(last_in, 10)


def on_device(sizes, query, cache_keys, cache_values, new_keys, new_values, page_map, page_table, lengths, out_weight):
    n_group, n_page, n_tensor = sizes
    slots, page, width = cache_keys.shape
    new_dev = new_keys.shape[0]
    seqs = query.shape[0]
    tokens = (slots + new_dev) * page
    kv_heads = width // HD
    share = query.shape[1] // HD // kv_heads
    rows = share * seqs
    n_sheet = n_page * CORES
    n_y = n_group // CORES
    columns = out_weight.shape[1]
    rows_a, rows_b = rows // n_group, rows // n_sheet
    bf16, f32 = jnp.bfloat16, jnp.float32
    scratch = [
        pltpu.VMEM(query.shape, bf16),
        pltpu.VMEM((tokens, width), bf16),
        pltpu.VMEM((tokens, width), bf16),
        pltpu.VMEM((2, page_map.shape[0]), jnp.int32),
        pltpu.VMEM(page_table.shape, jnp.int32),
        pltpu.VMEM((1, seqs), jnp.int32),
        pltpu.VMEM((columns, out_weight.shape[0]), bf16),
        pltpu.VMEM((new_dev, LANES), jnp.int32),
        pltpu.VMEM((seqs, tokens), f32),
        pltpu.VMEM((kv_heads, rows, tokens), f32),
        pltpu.VMEM((kv_heads, rows, tokens), bf16),
        pltpu.VMEM((kv_heads, rows, LANES), f32),
        pltpu.VMEM((n_group, rows_a, HD), bf16),
        pltpu.VMEM((n_sheet, rows_b, HD), bf16),
        pltpu.VMEM((n_group, 1, LANES), f32),
        pltpu.VMEM((n_sheet, 1, LANES), f32),
        pltpu.VMEM((n_group - 1, rows_a, HD), bf16),
        pltpu.VMEM((n_sheet - 1, rows_b, HD), bf16),
        pltpu.VMEM((n_group - 1, 1, LANES), f32),
        pltpu.VMEM((n_sheet - 1, 1, LANES), f32),
        pltpu.VMEM((rows_a, HD), bf16),
        pltpu.VMEM((rows_b, HD), bf16),
        pltpu.VMEM((1, LANES), f32),
        pltpu.VMEM((1, LANES), f32),
        pltpu.VMEM((n_page - 1, rows_a, HD), bf16),
        pltpu.VMEM((n_y - 1, rows_b, HD), bf16),
        pltpu.VMEM((n_page - 1, 1, LANES), f32),
        pltpu.VMEM((n_y - 1, 1, LANES), f32),
        pltpu.VMEM((n_group, rows_a, HD), bf16),
        pltpu.VMEM((n_sheet, rows_b, HD), bf16),
        pltpu.VMEM((columns, seqs), f32),
        pltpu.VMEM((n_tensor - 1, columns // n_tensor, seqs), f32),
        pltpu.SemaphoreType.DMA((9,)),
        pltpu.SemaphoreType.DMA((11,)),
        pltpu.SemaphoreType.DMA((11,)),
    ]
    return pl.pallas_call(
        functools.partial(kernel, (n_group, n_page, n_tensor, slots, new_dev)),
        out_shape=pltpu.VMEM((columns // n_tensor, seqs), bf16),
        in_specs=[pl.BlockSpec(memory_space=pltpu.HBM)] * 9,
        out_specs=pl.BlockSpec(memory_space=pltpu.VMEM),
        scratch_shapes=scratch,
        compiler_params=pltpu.CompilerParams(
            collective_id=0, has_side_effects=True, vmem_limit_bytes=40 * 1024 * 1024
        ),
    )(*[pltpu.with_memory_space_constraint(a, pltpu.HBM) for a in (
        query,
        cache_keys.reshape(slots * page, width),
        cache_values.reshape(slots * page, width),
        new_keys.reshape(new_dev * page, width),
        new_values.reshape(new_dev * page, width),
        page_map.T,
        page_table,
        lengths.reshape(1, seqs),
        out_weight.T,
    )]).T


def solution(mesh):
    shards = ("group", "page")
    sizes = (mesh.shape["group"], mesh.shape["page"], mesh.shape["tensor"])
    placed = (
        P(None, "tensor"),
        P(shards, None, "tensor"),
        P(shards, None, "tensor"),
        P(shards, None, "tensor"),
        P(shards, None, "tensor"),
        P(),
        P(),
        P(),
        P("tensor", shards),
    )
    return jax.shard_map(
        functools.partial(on_device, sizes),
        mesh=mesh,
        in_specs=placed,
        out_specs=P(None, ("group", "page", "tensor")),
        check_vma=False,
    )
```

```python
import functools
import math

import jax
import jax.numpy as jnp
from jax import lax
from jax.experimental import pallas as pl
from jax.experimental.pallas import tpu as pltpu
from jax.sharding import PartitionSpec as P

HD = 128
PAGE = 16
LANES = 128
CORES = 2
MESH = pl.DeviceIdType.MESH
VERY_LOW = -1.0e30
PVS = 2
SCALE2 = HD**-0.5 * math.log2(math.e)
NT = (((1,), (1,)), ((), ()))


def lanes_of(shape):
    return lax.broadcasted_iota(jnp.int32, shape, len(shape) - 1)


def rows_of(shape):
    return lax.broadcasted_iota(jnp.int32, shape, len(shape) - 2)


def lane_sum(x):
    return jnp.sum(x.astype(jnp.float32), axis=1, keepdims=True).astype(jnp.int32)


def lane_or(words):
    low = lane_sum(words & 0xFFFF)
    high = lane_sum(lax.shift_right_logical(words, 16) & 0xFFFF)
    return low, high


def build_bias(tbl, pm, lens, tgt, bias, gi, z, n_page, slots, new_dev):
    seqs, pages = tbl.shape
    total = pm.shape[1]
    shard = gi * n_page + z
    base = shard * slots
    eye = rows_of((seqs, seqs)) == lanes_of((seqs, seqs))
    length = lane_sum(jnp.where(eye, lens[...], 0))
    used = (length + (PAGE - 1)) >> 4
    fill = length - (used - 1) * PAGE
    target = pm[0:1, :]
    slot = pm[1:2, :]
    number = lanes_of((1, total))
    sheet = (number // new_dev) % n_page
    valid = (target == gi) & (sheet == z)
    off = shard * new_dev
    own = jnp.where(
        lanes_of((new_dev, total)) == rows_of((new_dev, total)) + off,
        (target * n_page + z) * slots + slot,
        0,
    )
    tgt[...] = jnp.broadcast_to(lane_sum(own), tgt.shape)
    stale = []
    for w in range(slots // 16):
        hit = valid & ((slot >> 4) == w)
        stale.append(lane_sum(jnp.where(hit, jnp.int32(1) << (slot & 15), 0)))
    shape = (seqs, LANES)
    used_b = jnp.broadcast_to(used, shape)
    words = [jnp.zeros(shape, jnp.int32) for _ in range(slots // 32)]
    fresh = jnp.zeros(shape, jnp.int16)
    last = jnp.zeros(shape, jnp.int32)
    marks = [jnp.broadcast_to(tgt[k : k + 1, :], shape) for k in range(new_dev)]
    narrow_marks = [m.astype(jnp.int16) for m in marks]
    narrow_bits = [jnp.int16((1 << k) if k < 15 else -(1 << 15)) for k in range(new_dev)]
    for c in range(pages // LANES):
        entry = tbl[:, c * LANES : (c + 1) * LANES]
        j = lanes_of(shape) + c * LANES
        last = last + jnp.where(j == used_b - 1, entry, 0)
        entry = jnp.where(j < used_b, entry, -1)
        local = entry - base
        high = local >> 5
        bit = jnp.int32(1) << (local & 31)
        for w in range(slots // 32):
            words[w] = words[w] | jnp.where(high == w, bit, 0)
        narrow = entry.astype(jnp.int16)
        for k in range(new_dev):
            fresh = fresh | jnp.where(narrow == narrow_marks[k], narrow_bits[k], jnp.int16(0))
    last_b = jnp.broadcast_to(lane_sum(last), shape)
    fill_b = jnp.broadcast_to(fill, shape)
    owned = []
    for w in range(slots // 32):
        owned.extend(lane_or(words[w]))
    fresh_b = jnp.broadcast_to(lane_sum(fresh.astype(jnp.int32) & 0xFFFF), shape)
    last_fresh = jnp.zeros(shape, jnp.int32)
    for k in range(new_dev):
        last_fresh = last_fresh | jnp.where(last_b == marks[k], 1 << k, 0)
    lane = lanes_of(shape)
    tail_end = (last_b - base) * PAGE + PAGE
    tail_start = tail_end - PAGE + fill_b
    per_tile = LANES // PAGE
    for w in range(slots // 16):
        word = jnp.broadcast_to(owned[w] & ~stale[w], shape)
        for half in range(16 // per_tile):
            c = w * (16 // per_tile) + half
            token = lane + c * LANES
            here = (lax.shift_right_logical(word, (lane >> 4) + half * per_tile) & 1) == 1
            here = here & ((token < tail_start) | (token >= tail_end))
            bias[:, c * LANES : (c + 1) * LANES] = jnp.where(here, 0.0, VERY_LOW)
    first = slots * PAGE
    for c in range(new_dev // per_tile):
        shift = (lane >> 4) + c * per_tile
        here = (lax.shift_right_logical(fresh_b, shift) & 1) == 1
        ends = (lax.shift_right_logical(last_fresh, shift) & 1) == 1
        here = here & ~(ends & ((lane & 15) >= fill_b))
        bias[:, first + c * LANES : first + (c + 1) * LANES] = jnp.where(here, 0.0, VERY_LOW)


def merge(stat_rows, values, rows):
    count = len(stat_rows)
    pad = [jnp.zeros((-count % 8, LANES), jnp.float32)] if count % 8 else []
    stats = jnp.concatenate(stat_rows + pad, axis=0)
    real = rows_of(stats.shape) < count
    highest = jnp.max(jnp.where(real, stats, -jnp.inf), axis=0, keepdims=True)
    in_max = lanes_of(stats.shape) < rows
    factor = jnp.where(real & in_max, jnp.exp2(jnp.where(in_max, stats - highest, 0.0)), 0.0)
    sums = pltpu.roll(stats, LANES - rows, 1)
    total = jnp.sum(factor * jnp.where(in_max, sums, 0.0), axis=0, keepdims=True)
    square = jnp.concatenate(
        [factor, jnp.broadcast_to(total, (8, LANES)), jnp.zeros((LANES - 8 - stats.shape[0], LANES), jnp.float32)],
        axis=0,
    )
    across = square.T
    mixed = across[:rows, 0:1] * values[0].astype(jnp.float32)
    for k in range(1, count):
        mixed = mixed + across[:rows, k : k + 1] * values[k].astype(jnp.float32)
    total_column = across[:rows, stats.shape[0] : stats.shape[0] + 1]
    return highest, total, total_column, mixed


def kernel(
    dims,
    q_in,
    ck_in,
    cv_in,
    nk_in,
    nv_in,
    pm_in,
    tbl_in,
    len_in,
    w_in,
    out_ref,
    q,
    key,
    value,
    pm,
    tbl,
    lens,
    weight,
    tgt,
    bias,
    scores,
    probs,
    tops,
    part_a,
    part_b,
    stat_a,
    stat_b,
    got_a,
    got_b,
    gots_a,
    gots_b,
    mid_a,
    mid_b,
    mids_a,
    mids_b,
    gotm_a,
    gotm_b,
    gotms_a,
    gotms_b,
    att_a,
    att_b,
    last_out,
    last_in,
    local_sem,
    send_sem,
    recv_sem,
):
    n_group, n_page, n_tensor, slots, new_dev = dims
    n_y = n_group // CORES
    gi = lax.axis_index("group")
    z = lax.axis_index("page")
    x = lax.axis_index("tensor")
    y = lax.div(gi, CORES)
    core = lax.rem(gi, CORES)
    seqs = q.shape[0]
    kv_heads = key.shape[1] // HD
    share = q.shape[1] // HD // kv_heads
    rows = share * seqs
    cache_rows = slots * PAGE

    copies = []

    def fetch(src, dst):
        copy = pltpu.make_async_copy(src, dst, local_sem.at[len(copies)])
        copy.start()
        copies.append(copy)

    fetch(len_in, lens)
    fetch(pm_in, pm)
    fetch(tbl_in, tbl)
    fetch(q_in, q)
    fetch(ck_in, key.at[pl.ds(0, cache_rows)])
    fetch(nk_in, key.at[pl.ds(cache_rows, new_dev * PAGE)])
    fetch(cv_in, value.at[pl.ds(0, cache_rows)])
    fetch(nv_in, value.at[pl.ds(cache_rows, new_dev * PAGE)])
    fetch(w_in, weight)

    def along_group(d):
        return {"group": lax.rem(gi + d, n_group)}

    def along_sheet(d):
        other = lax.rem(z * CORES + core + d, n_page * CORES)
        return {"group": y * CORES + lax.rem(other, CORES), "page": lax.div(other, CORES)}

    def along_page(d):
        return {"page": lax.rem(z + d, n_page)}

    def along_y(d):
        return {"group": lax.rem(y + d, n_y) * CORES + core}

    def along_tensor(d):
        return {"tensor": lax.rem(x + d, n_tensor)}

    n_sheet = n_page * CORES
    place_b = z * CORES + core
    barrier = pltpu.get_barrier_semaphore()

    def other_core(place, d, count):
        return lax.rem(place + d, count) * CORES + 1 - core

    peers = []
    for d in range(1, n_page):
        hops = min(d, n_page - d)
        peers.append((hops, along_page(d)))
        peers.append((hops, {"group": y * CORES + 1 - core, "page": lax.rem(z + d, n_page)}))
    for d in range(1, n_y):
        hops = min(d, n_y - d)
        peers.append((hops, along_y(d)))
        peers.append((hops, {"group": other_core(y, d, n_y)}))
    peers += [(min(d, n_tensor - d), along_tensor(d)) for d in range(1, n_tensor)]
    peers.append((0, {"group": y * CORES + 1 - core}))
    for _, peer in sorted(peers, key=lambda p: -p[0]):
        pl.semaphore_signal(barrier, inc=1, device_id=peer, device_id_type=MESH)

    def send(src, dst, peer, at):
        pltpu.make_async_remote_copy(
            src_ref=src,
            dst_ref=dst,
            send_sem=send_sem.at[at],
            recv_sem=recv_sem.at[at],
            device_id=peer,
            device_id_type=MESH,
        ).start()

    def received(ref, at):
        pltpu.make_async_copy(ref, ref, recv_sem.at[at]).wait()

    def left(ref, at):
        pltpu.make_async_copy(ref, ref, send_sem.at[at]).wait()

    for k in range(3):
        copies[k].wait()
    build_bias(tbl, pm, lens, tgt, bias, gi, z, n_page, slots, new_dev)
    for k in range(3, 6):
        copies[k].wait()

    def score(half):
        heads = range(half * share, (half + 1) * share)
        stacked = jnp.concatenate([q[:, h * HD : (h + 1) * HD] for h in heads], axis=0)
        s = lax.dot_general(
            stacked,
            key[:, half * HD : (half + 1) * HD],
            NT,
            preferred_element_type=jnp.float32,
        )
        for h in range(share):
            at = slice(h * seqs, (h + 1) * seqs)
            scores[half, at, :] = s[at, :] * SCALE2 + bias[...]

    def far_first(count):
        return sorted(range(1, count), key=lambda d: -min(d, count - d))

    def soften(half):
        block = 16
        for b in range(rows // block):
            at = slice(b * block, (b + 1) * block)
            s = scores[half, at, :]
            top = jnp.max(s, axis=1, keepdims=True)
            probs[half, at, :] = jnp.exp2(s - top).astype(jnp.bfloat16)
            tops[half, at, :] = jnp.broadcast_to(top, (block, LANES))

    def weigh(half, part, stat):
        count, own_rows = part.shape[0], part.shape[1]
        v = value[:, half * HD : (half + 1) * HD]
        wide = jnp.concatenate([v, jnp.ones_like(v)], axis=1)
        summed = jnp.concatenate(
            [
                jnp.dot(probs[half, i * rows // PVS : (i + 1) * rows // PVS, :], wide, preferred_element_type=jnp.float32)
                for i in range(PVS)
            ],
            axis=0,
        )
        shape = (own_rows, LANES)
        lane, row = lanes_of(shape), rows_of(shape)
        for k in range(count):
            at = slice(k * own_rows, (k + 1) * own_rows)
            part[k] = summed[at, :HD].astype(jnp.bfloat16)
            sums = jnp.where(lane == row + own_rows, summed[at, HD:], 0.0)
            picked = jnp.where(lane == row, tops[half, at, :], sums)
            stat[k] = jnp.sum(picked, axis=0, keepdims=True)

    def near_root(count):
        return sorted(range(count), key=lambda k: min(k, count - k))

    def scatter(part, stat, got, gots, place, peer_at, at):
        count = part.shape[0]
        for k in reversed(near_root(count // CORES)):
            for c in range(CORES):
                spot = k * CORES + c

                @pl.when(place != spot)
                def _():
                    slot = lax.rem(spot - place + count, count) - 1
                    send(part.at[spot], got.at[slot], peer_at(k, c), at)
                    send(stat.at[spot], gots.at[slot], peer_at(k, c), at + 1)

    def merge_scattered(part, stat, got, gots, mid, mids, place, at):
        count, own_rows = part.shape[0], part.shape[1]
        received(got, at)
        received(gots, at + 1)
        stats = [stat[place]] + [gots[d - 1] for d in range(1, count)]
        values = [part[place]] + [got[d - 1] for d in range(1, count)]
        highest, total, _, mixed = merge(stats, values, own_rows)
        mid[...] = mixed.astype(jnp.bfloat16)
        low = lanes_of((1, LANES)) < own_rows
        mids[...] = jnp.where(low, highest, pltpu.roll(total, own_rows, 1))

    def spread(mid, mids, gotm, gotms, place, peer_at, at):
        count = gotm.shape[0] + 1
        for k in near_root(count):

            @pl.when(place != k)
            def _():
                slot = lax.rem(k - place + count, count) - 1
                send(mid, gotm.at[slot], peer_at(k), at)
                send(mids, gotms.at[slot], peer_at(k), at + 1)

    def merge_spread(mid, mids, gotm, gotms, att, place, at):
        received(gotm, at)
        received(gotms, at + 1)
        others = range(gotm.shape[0])
        stats = [mids[...]] + [gotms[k] for k in others]
        values = [mid[...]] + [gotm[k] for k in others]
        _, _, total_column, mixed = merge(stats, values, mid.shape[0])
        att[place] = (mixed / total_column).astype(jnp.bfloat16)

    def gather(att, place, peer_at, at):
        count = att.shape[0]
        for k in near_root(count // CORES):
            for c in (1, 0):
                spot = k * CORES + c

                @pl.when(place != spot)
                def _():
                    send(att.at[place], att.at[place], peer_at(k, c), at)

    score(1)
    soften(1)
    for k in range(6, 8):
        copies[k].wait()
    weigh(1, part_b, stat_b)
    pl.semaphore_wait(barrier, len(peers))
    scatter(part_b, stat_b, got_b, gots_b, place_b, lambda k, c: {"group": y * CORES + c, "page": k}, 2)
    score(0)
    soften(0)
    weigh(0, part_a, stat_a)
    scatter(part_a, stat_a, got_a, gots_a, gi, lambda k, c: {"group": k * CORES + c}, 0)
    merge_scattered(part_b, stat_b, got_b, gots_b, mid_b, mids_b, place_b, 2)
    spread(mid_b, mids_b, gotm_b, gotms_b, y, lambda k: {"group": k * CORES + core}, 6)
    merge_scattered(part_a, stat_a, got_a, gots_a, mid_a, mids_a, gi, 0)
    spread(mid_a, mids_a, gotm_a, gotms_a, z, lambda k: {"page": k}, 4)
    left(got_a, 0)
    left(gots_a, 1)
    left(got_b, 2)
    left(gots_b, 3)
    merge_spread(mid_b, mids_b, gotm_b, gotms_b, att_b, place_b, 6)
    gather(att_b, place_b, lambda k, c: {"group": y * CORES + c, "page": k}, 9)
    merge_spread(mid_a, mids_a, gotm_a, gotms_a, att_a, gi, 4)
    gather(att_a, gi, lambda k, c: {"group": k * CORES + c}, 8)
    left(gotm_a, 4)
    left(gotms_a, 5)
    left(gotm_b, 6)
    left(gotms_b, 7)
    others_a = att_a.at[pl.ds(0, n_group - 1)]
    others_b = att_b.at[pl.ds(0, n_sheet - 1)]
    copies[8].wait()

    def project(att, first):
        flat = att[...].reshape(rows, HD)
        features = jnp.concatenate([flat[h * seqs : (h + 1) * seqs] for h in range(share)], axis=1)
        block = weight[:, first * HD : (first + share) * HD]
        return lax.dot_general(block, features, NT, preferred_element_type=jnp.float32)

    received(others_b, 9)
    last_out[...] = project(att_b, share)
    received(others_a, 8)
    last_out[...] += project(att_a, 0)
    width = out_ref.shape[0]

    def block_of(d):
        return last_out.at[pl.ds(pl.multiple_of(lax.rem(x + d, n_tensor) * width, width), width)]

    for d in far_first(n_tensor):
        send(block_of(d), last_in.at[d - 1], along_tensor(d), 10)
    left(others_a, 8)
    left(others_b, 9)
    received(last_in, 10)
    result = block_of(0)[...]
    for d in range(1, n_tensor):
        result = result + last_in[d - 1]
    out_ref[...] = result.astype(out_ref.dtype)
    left(last_in, 10)


def on_device(sizes, query, cache_keys, cache_values, new_keys, new_values, page_map, page_table, lengths, out_weight):
    n_group, n_page, n_tensor = sizes
    slots, page, width = cache_keys.shape
    new_dev = new_keys.shape[0]
    seqs = query.shape[0]
    tokens = (slots + new_dev) * page
    kv_heads = width // HD
    share = query.shape[1] // HD // kv_heads
    rows = share * seqs
    n_sheet = n_page * CORES
    n_y = n_group // CORES
    columns = out_weight.shape[1]
    rows_a, rows_b = rows // n_group, rows // n_sheet
    bf16, f32 = jnp.bfloat16, jnp.float32
    scratch = [
        pltpu.VMEM(query.shape, bf16),
        pltpu.VMEM((tokens, width), bf16),
        pltpu.VMEM((tokens, width), bf16),
        pltpu.VMEM((2, page_map.shape[0]), jnp.int32),
        pltpu.VMEM(page_table.shape, jnp.int32),
        pltpu.VMEM((1, seqs), jnp.int32),
        pltpu.VMEM((columns, out_weight.shape[0]), bf16),
        pltpu.VMEM((new_dev, LANES), jnp.int32),
        pltpu.VMEM((seqs, tokens), f32),
        pltpu.VMEM((kv_heads, rows, tokens), f32),
        pltpu.VMEM((kv_heads, rows, tokens), bf16),
        pltpu.VMEM((kv_heads, rows, LANES), f32),
        pltpu.VMEM((n_group, rows_a, HD), bf16),
        pltpu.VMEM((n_sheet, rows_b, HD), bf16),
        pltpu.VMEM((n_group, 1, LANES), f32),
        pltpu.VMEM((n_sheet, 1, LANES), f32),
        pltpu.VMEM((n_group - 1, rows_a, HD), bf16),
        pltpu.VMEM((n_sheet - 1, rows_b, HD), bf16),
        pltpu.VMEM((n_group - 1, 1, LANES), f32),
        pltpu.VMEM((n_sheet - 1, 1, LANES), f32),
        pltpu.VMEM((rows_a, HD), bf16),
        pltpu.VMEM((rows_b, HD), bf16),
        pltpu.VMEM((1, LANES), f32),
        pltpu.VMEM((1, LANES), f32),
        pltpu.VMEM((n_page - 1, rows_a, HD), bf16),
        pltpu.VMEM((n_y - 1, rows_b, HD), bf16),
        pltpu.VMEM((n_page - 1, 1, LANES), f32),
        pltpu.VMEM((n_y - 1, 1, LANES), f32),
        pltpu.VMEM((n_group, rows_a, HD), bf16),
        pltpu.VMEM((n_sheet, rows_b, HD), bf16),
        pltpu.VMEM((columns, seqs), f32),
        pltpu.VMEM((n_tensor - 1, columns // n_tensor, seqs), f32),
        pltpu.SemaphoreType.DMA((9,)),
        pltpu.SemaphoreType.DMA((11,)),
        pltpu.SemaphoreType.DMA((11,)),
    ]
    return pl.pallas_call(
        functools.partial(kernel, (n_group, n_page, n_tensor, slots, new_dev)),
        out_shape=pltpu.VMEM((columns // n_tensor, seqs), bf16),
        in_specs=[pl.BlockSpec(memory_space=pltpu.HBM)] * 9,
        out_specs=pl.BlockSpec(memory_space=pltpu.VMEM),
        scratch_shapes=scratch,
        compiler_params=pltpu.CompilerParams(
            collective_id=0, has_side_effects=True, vmem_limit_bytes=40 * 1024 * 1024
        ),
    )(*[pltpu.with_memory_space_constraint(a, pltpu.HBM) for a in (
        query,
        cache_keys.reshape(slots * page, width),
        cache_values.reshape(slots * page, width),
        new_keys.reshape(new_dev * page, width),
        new_values.reshape(new_dev * page, width),
        page_map.T,
        page_table,
        lengths.reshape(1, seqs),
        out_weight.T,
    )]).T


def solution(mesh):
    shards = ("group", "page")
    sizes = (mesh.shape["group"], mesh.shape["page"], mesh.shape["tensor"])
    placed = (
        P(None, "tensor"),
        P(shards, None, "tensor"),
        P(shards, None, "tensor"),
        P(shards, None, "tensor"),
        P(shards, None, "tensor"),
        P(),
        P(),
        P(),
        P("tensor", shards),
    )
    return jax.shard_map(
        functools.partial(on_device, sizes),
        mesh=mesh,
        in_specs=placed,
        out_specs=P(None, ("group", "page", "tensor")),
        check_vma=False,
    )
```
